256 devices in a mesh: row: 8 (over x, y_hi), col: 32 (over z, y_lo, core).
Axes of the slice: x: 4, y: 4 (y_hi: 2, y_lo: 2; y = y_hi * 2 + y_lo), z: 8, core: 2. Of those that a mesh axis runs over, the one named last changes fastest.
Arguments:
- e_field: float32 [3, 64, 64, 4096], P(None, None, 'row', 'col'), may hold values from -6 to 6
- h_field: float32 [3, 64, 64, 4096], P(None, None, 'row', 'col'), may hold values from -6 to 6
- e_coef: float32 [64, 64, 4096], P(None, 'row', 'col'), may hold values from 0.125 to 0.5
- basis: float32 [128, 64, 4096], P('row', None, 'col'), may hold values from -0.01171875 to 0.01171875
- pml_width: int32 [4], replicated, may hold values from 2 to 8
- snap_index: int32 [64], replicated, may hold values from 0 to 383
Outputs:
- e_final: float32 [3, 64, 64, 4096], P(None, None, 'row', 'col')
- h_final: float32 [3, 64, 64, 4096], P(None, None, 'row', 'col')
- coefficients: float32 [64, 128], replicated
- gram: float32 [64, 64], replicated
The draws below stay inside these ranges and needn't reach their ends.
All inputs are finite; a program needn't handle non-finite values.
Results may differ from the reference program's by a relative error of at most 0.00008.
Values sent between devices are 32-bit elements; how exact they have to be, the bound alone decides.
A program may use at most 64 MiB of HBM per device.

```python
import math
import jax
import jax.numpy as jnp
from jax import lax

NZ = 64
STEPS = 8
RANK = 128
SNAPS = 64
NX = 64
NY = 4096


def place_ends(entries, own_key, low, high):
    spot = [jax.random.randint(jax.random.fold_in(own_key, axis), (), 0, length) for axis, length in enumerate(entries.shape)]
    main_axis = entries.shape.index(max(entries.shape))
    next_to = spot[:main_axis] + [(spot[main_axis] + 1) % entries.shape[main_axis]] + spot[main_axis + 1:]
    return entries.at[tuple(spot)].set(low).at[tuple(next_to)].set(high)


def level_of(rng, shape, shards, smallest, top_value):
    level, own = 1.0, jax.random.fold_in(rng, 6)
    for position, blocks in shards:
        draws = jnp.exp(jax.random.uniform(jax.random.fold_in(own, position), (blocks,), jnp.float32, smallest / len(shards), top_value / len(shards)))
        level = level * jnp.repeat(draws, shape[position] // blocks).reshape([-1 if axis == position else 1 for axis in range(len(shape))])
    return level


def normal_values(own_key, dims, width, limit, cuts=(), held_as=jnp.bfloat16):
    result = jax.random.normal(own_key, dims, jnp.float32) * width
    if len(cuts) > 0:
        result = level_of(own_key, dims, cuts, -0.22, 0.18) * result
    return jnp.clip(result, min=-limit, max=limit).astype(held_as)


def setup_inputs(seed: int = 0) -> dict:
    key_list = jax.random.split(jax.random.key(seed), 7)
    e_field = normal_values(key_list[0], (3, NZ, NX, NY), 1.0, 6.0, ((2, 8), (3, 32)), jnp.float32)
    h_field = normal_values(key_list[1], (3, NZ, NX, NY), 1.0, 6.0, ((2, 8), (3, 32)), jnp.float32)
    e_coef = jnp.clip(jnp.exp(math.log(0.5) - 1.3862944 * jax.random.uniform(key_list[2], (NZ, NX, NY), jnp.float32) ** level_of(key_list[2], (NZ, NX, NY), ((1, 8), (2, 32)), -0.2, 0.2)), 0.125, 0.5)
    basis = normal_values(key_list[3], (RANK, NX, NY), (NX * NY) ** -0.5, 0.01171875, ((0, 8), (2, 32)), jnp.float32)
    pml_width = place_ends(jax.random.randint(key_list[4], (4,), 2, 9), jax.random.fold_in(key_list[4], 1), 2, 8).astype(jnp.int32)
    snap_index = place_ends(jax.random.randint(key_list[5], (SNAPS,), 0, 6 * NZ), jax.random.fold_in(key_list[5], 1), 0, (6 * NZ) - 1).astype(jnp.int32)
    return {"e_field": e_field, "h_field": h_field, "e_coef": e_coef, "basis": basis, "pml_width": pml_width, "snap_index": snap_index}


time_step = 0.5
sigma_top = 4.0
alpha_shift = 0.05


def forward(field, axis, plane):
    count = field.shape[axis]
    after = jnp.concatenate([lax.slice_in_dim(field, 1, count, axis=axis), jnp.expand_dims(plane, axis)], axis)
    return after - field


def backward(field, axis, plane):
    count = field.shape[axis]
    before = jnp.concatenate([jnp.expand_dims(plane, axis), lax.slice_in_dim(field, 0, count - 1, axis=axis)], axis)
    return field - before


def absorber(positions, total, low, high):
    depth = jnp.maximum(jnp.maximum((low - positions) / low, (positions - (total - 1.0 - high)) / high), 0.0)
    sigma = sigma_top * depth ** 3
    damp = jnp.exp(-(sigma + alpha_shift) * time_step)
    gain = sigma / (sigma + alpha_shift) * (damp - 1.0)
    return damp, gain


def magnetic(e_field, h_field, psi, next_x, next_y, damp_x, gain_x, damp_y, gain_y):
    e_x, e_y, e_z = e_field[0], e_field[1], e_field[2]
    h_x, h_y, h_z = h_field[0], h_field[1], h_field[2]
    zplane = jnp.zeros_like(e_x[0])
    ez_dy = forward(e_z, 2, next_y[1])
    ey_dz = forward(e_y, 0, zplane)
    ex_dz = forward(e_x, 0, zplane)
    ez_dx = forward(e_z, 1, next_x[1])
    ey_dx = forward(e_y, 1, next_x[0])
    ex_dy = forward(e_x, 2, next_y[0])
    psi_hxy = damp_y * psi[0] + gain_y * ez_dy
    psi_hyx = damp_x * psi[1] + gain_x * ez_dx
    psi_hzx = damp_x * psi[2] + gain_x * ey_dx
    psi_hzy = damp_y * psi[3] + gain_y * ex_dy
    h_x = h_x - time_step * (ez_dy + psi_hxy - ey_dz)
    h_y = h_y - time_step * (ex_dz - ez_dx - psi_hyx)
    h_z = h_z - time_step * (ey_dx + psi_hzx - ex_dy - psi_hzy)
    return jnp.stack((h_x, h_y, h_z)), (psi_hxy, psi_hyx, psi_hzx, psi_hzy)


def electric(e_field, h_field, psi, e_coef, prev_x, prev_y, damp_x, gain_x, damp_y, gain_y):
    e_x, e_y, e_z = e_field[0], e_field[1], e_field[2]
    h_x, h_y, h_z = h_field[0], h_field[1], h_field[2]
    zplane = jnp.zeros_like(h_x[0])
    hz_dy = backward(h_z, 2, prev_y[1])
    hy_dz = backward(h_y, 0, zplane)
    hx_dz = backward(h_x, 0, zplane)
    hz_dx = backward(h_z, 1, prev_x[1])
    hy_dx = backward(h_y, 1, prev_x[0])
    hx_dy = backward(h_x, 2, prev_y[0])
    psi_exy = damp_y * psi[0] + gain_y * hz_dy
    psi_eyx = damp_x * psi[1] + gain_x * hz_dx
    psi_ezx = damp_x * psi[2] + gain_x * hy_dx
    psi_ezy = damp_y * psi[3] + gain_y * hx_dy
    e_x = e_x + e_coef * (hz_dy + psi_exy - hy_dz)
    e_y = e_y + e_coef * (hx_dz - hz_dx - psi_eyx)
    e_z = e_z + e_coef * (hy_dx + psi_ezx - hx_dy - psi_ezy)
    return jnp.stack((e_x, e_y, e_z)), (psi_exy, psi_eyx, psi_ezx, psi_ezy)


def reference(e_field, h_field, e_coef, basis, pml_width, snap_index):
    widths = pml_width.astype(jnp.float32)
    x_pos = jnp.arange(NX, dtype=jnp.float32)
    y_pos = jnp.arange(NY, dtype=jnp.float32)
    hdx, hgx = absorber(x_pos + 0.5, float(NX), widths[0], widths[1])
    hdy, hgy = absorber(y_pos + 0.5, float(NY), widths[2], widths[3])
    edx, egx = absorber(x_pos, float(NX), widths[0], widths[1])
    edy, egy = absorber(y_pos, float(NY), widths[2], widths[3])
    hdx, hgx, edx, egx = [v.reshape(1, NX, 1) for v in (hdx, hgx, edx, egx)]
    hdy, hgy, edy, egy = [v.reshape(1, 1, NY) for v in (hdy, hgy, edy, egy)]
    zeros_cells = jnp.zeros((NZ, NX, NY), jnp.float32)
    psi_mag = (zeros_cells,) * 4
    psi_ele = (zeros_cells,) * 4
    plane_x = jnp.zeros((2, NZ, NY), jnp.float32)
    plane_y = jnp.zeros((2, NZ, NX), jnp.float32)
    for step in range(STEPS):
        h_field, psi_mag = magnetic(e_field, h_field, psi_mag, plane_x, plane_y, hdx, hgx, hdy, hgy)
        e_field, psi_ele = electric(e_field, h_field, psi_ele, e_coef, plane_x, plane_y, edx, egx, edy, egy)
    planes = jnp.concatenate((e_field, h_field), 0).reshape(6 * NZ, NX, NY)
    snaps = jnp.take(planes, snap_index, axis=0).reshape(SNAPS, NX * NY)
    coefficients = jnp.dot(snaps, basis.reshape(RANK, NX * NY).T, precision=lax.Precision.HIGHEST)
    gram = jnp.dot(snaps, snaps.T, precision=lax.Precision.HIGHEST) / float(NX * NY)
    return e_field, h_field, coefficients, gram
```

```python
import functools

import jax
import jax.numpy as jnp
from jax import lax
from jax.experimental import pallas as pl
from jax.experimental.pallas import tpu as pltpu
from jax.sharding import PartitionSpec as P

STEPS = 8
time_step = 0.5
sigma_top = 4.0
alpha_shift = 0.05
MESH = pl.DeviceIdType.MESH
TILE = (8, 128)
f32 = jnp.float32


def absorber(positions, total, low, high):
    depth = jnp.maximum(
        jnp.maximum((low - positions) / low, (positions - (total - 1.0 - high)) / high), 0.0
    )
    sigma = sigma_top * (depth * depth * depth)
    damp = jnp.exp(-(sigma + alpha_shift) * time_step)
    gain = sigma / (sigma + alpha_shift) * (damp - 1.0)
    return damp, gain


def kernel(
    n_row, n_col, nz, unroll,
    e_in, h_in, c_in, basis, pml, snap,
    e_out, h_out, coef_out, gram_out,
    F, CE, PSI, K,
    sxd, sxu, syd, syu, scb,
    rxd, rxu, ryd, ryu, rca, rcb,
    W, R, RA, PB, G,
    in_sem, out_sem, hs_sem, hr_sem, bs_sem, br_sem, own_sem,
    as_sem, ar_sem, ps_sem, pr_sem, gs_sem, gr_sem,
):
    row = lax.axis_index("row")
    col = lax.axis_index("col")
    n_a, n_b = n_row * 2, n_col // 2
    y_lo = lax.rem(lax.div(col, 2), 2)
    a_me = row * 2 + y_lo
    b_me = lax.div(col, 4) * 2 + lax.rem(col, 2)

    def a_device(m):
        return (lax.div(m, 2), lax.div(col, 4) * 4 + lax.rem(m, 2) * 2 + lax.rem(col, 2))

    def b_device(m):
        return (row, lax.div(m, 2) * 4 + y_lo * 2 + lax.rem(m, 2))

    loads = [
        pltpu.make_async_copy(e_in, F.at[0:3], in_sem.at[0]),
        pltpu.make_async_copy(h_in, F.at[3:6], in_sem.at[1]),
        pltpu.make_async_copy(c_in, CE, in_sem.at[2]),
    ]
    for copy in loads:
        copy.start()
    modes_here = basis.shape[0]

    def own_modes():
        return pltpu.make_async_copy(
            basis.at[:, pl.ds(pl.multiple_of(row * 8, 8), 8), :],
            W.at[pl.ds(row * modes_here, modes_here)],
            own_sem.at[0],
        )

    own_modes().start()

    barrier = pltpu.get_barrier_semaphore()

    def greet(device):
        pl.semaphore_signal(barrier, inc=1, device_id=device, device_id_type=MESH)

    @pl.loop(1, n_a)
    def _(j):
        greet(a_device(lax.rem(a_me + j, n_a)))

    @pl.loop(1, n_b)
    def _(j):
        greet(b_device(lax.rem(b_me + j, n_b)))

    up_x, dn_x = row < n_row - 1, row > 0
    up_y, dn_y = col < n_col - 1, col > 0
    ca_out, ca_in = up_x & dn_y, dn_x & up_y

    @pl.when(up_y)
    def _():
        greet((row, col + 1))

    @pl.when(dn_y)
    def _():
        greet((row, col - 1))

    @pl.when(ca_out)
    def _():
        greet((row + 1, col - 1))

    @pl.when(ca_in)
    def _():
        greet((row - 1, col + 1))

    greeted = n_a - 1 + n_b - 1
    for flag in (up_y, dn_y, ca_out, ca_in):
        greeted = greeted + flag.astype(jnp.int32)

    sub = lax.broadcasted_iota(jnp.int32, TILE, 0)
    lane = lax.broadcasted_iota(jnp.int32, TILE, 1)
    w = [jnp.full(TILE, pml[i], jnp.int32).astype(f32) for i in range(4)]
    x_pos = (row * 8 + sub).astype(f32)
    y_pos = (col * 128 + lane).astype(f32)
    full_x, full_y = float(n_row * 8), float(n_col * 128)
    hdx, hgx = absorber(x_pos + 0.5, full_x, w[0], w[1])
    hdy, hgy = absorber(y_pos + 0.5, full_y, w[2], w[3])
    edx, egx = absorber(x_pos, full_x, w[0], w[1])
    edy, egy = absorber(y_pos, full_y, w[2], w[3])
    _, gxm = absorber((row * 8 - 1 + 0 * sub).astype(f32) + 0.5, full_x, w[0], w[1])
    _, gym = absorber((col * 128 - 1 + 0 * lane).astype(f32) + 0.5, full_y, w[2], w[3])
    s7, s0, l127, l0 = sub == 7, sub == 0, lane == 127, lane == 0
    zero = jnp.zeros(TILE, f32)
    coeffs = [
        hdx, hgx, hdy, hgy, edx, egx, edy, egy,
        jnp.where(s7, 0.5 * (1.0 + hgx), zero), jnp.where(s7, hgx, zero),
        jnp.where(l127, 0.5 * (1.0 + hgy), zero), jnp.where(l127, hgy, zero),
        0.5 * (1.0 + gxm) * dn_x.astype(f32), 0.5 * (1.0 + gym) * dn_y.astype(f32),
    ]
    for i, value in enumerate(coeffs):
        K[i] = value
    HDX, HGX, HDY, HGY, EDX, EGX, EDY, EGY, CXU, PXU, CYU, PYU, CXD, CYD = range(14)

    @pl.loop(0, nz)
    def _(z):
        for i in range(8):
            PSI[i, z] = zero

    def clear(ref, wanted):
        @pl.when(wanted)
        def _():
            @pl.loop(0, STEPS)
            def _(n):
                ref[n] = jnp.zeros(ref.shape[1:], f32)

    clear(rxd, ~up_x)
    clear(rxu, ~dn_x)
    clear(ryd, ~up_y)
    clear(ryu, ~dn_y)
    clear(rca, ~ca_in)
    clear(rcb, ~ca_out)

    def row_of(ref, n, c, z):
        return jnp.broadcast_to(ref[n, c, pl.ds(z, 1), :], TILE)

    def roll_l(v, by):
        return pltpu.roll(v, by, 1)

    def roll_s(v, by):
        return pltpu.roll(v, by, 0)

    def partial_h(E, H, psi, ex_next, ey_next):
        ex, ey, ez = E
        hx, hy, hz = H
        ez_dy = jnp.where(l127, 0.0, roll_l(ez, 127)) - ez
        ex_dy = jnp.where(l127, 0.0, roll_l(ex, 127)) - ex
        ez_dx = jnp.where(s7, 0.0, roll_s(ez, 7)) - ez
        ey_dx = jnp.where(s7, 0.0, roll_s(ey, 7)) - ey
        ey_dz = ey_next - ey
        ex_dz = ex_next - ex
        p0 = K[HDY] * psi[0] + K[HGY] * ez_dy
        p1 = K[HDX] * psi[1] + K[HGX] * ez_dx
        p2 = K[HDX] * psi[2] + K[HGX] * ey_dx
        p3 = K[HDY] * psi[3] + K[HGY] * ex_dy
        hx = hx - time_step * (ez_dy + p0 - ey_dz)
        hy = hy - time_step * (ex_dz - ez_dx - p1)
        hz = hz - time_step * (ey_dx + p2 - ex_dy - p3)
        return (hx, hy, hz), (p0, p1, p2, p3)

    def pack_e(n, z, E, pd, pb):
        ex, ey, ez = E
        sxd[n, 0, pl.ds(z, 1), :] = ey[0:1, :]
        sxd[n, 1, pl.ds(z, 1), :] = ez[0:1, :]
        low, high = lane == z, lane == 64 + z
        pd = jnp.where(low, roll_l(ex, z), jnp.where(high, roll_l(ez, 64 + z), pd))
        pb = jnp.where(high, roll_l(ey, lax.rem(65 + z, 128)), pb)
        return pd, pb

    def finish_h(n, z, E, H, psi, ex_next, ey_next, pu):
        H, psi = partial_h(E, H, psi, ex_next, ey_next)
        for i in range(3):
            F[3 + i, z] = H[i]
        for i in range(4):
            PSI[i, z] = psi[i]
        sxu[n, 0, pl.ds(z, 1), :] = H[1][7:8, :]
        sxu[n, 1, pl.ds(z, 1), :] = H[2][7:8, :]
        low, high = lane == z, lane == 64 + z
        return jnp.where(
            low, roll_l(H[0], z + 1), jnp.where(high, roll_l(H[2], lax.rem(65 + z, 128)), pu)
        )

    def electric(n, z, yd, yu, ca, hx_prev, hy_prev):
        ex, ey, ez = F[0, z], F[1, z], F[2, z]
        hx, hy, hz = F[3, z], F[4, z], F[5, z]
        p0, p1, p2, p3 = PSI[0, z], PSI[1, z], PSI[2, z], PSI[3, z]
        ey8, ez8 = row_of(rxd, n, 0, z), row_of(rxd, n, 1, z)
        ex128, ez128 = roll_l(yd, 127 - z), roll_l(yd, 63 - z)
        hy = hy + K[CXU] * ez8
        p1 = p1 + K[PXU] * ez8
        hx = hx - K[CYU] * ez128
        p0 = p0 + K[PYU] * ez128
        hz = hz - K[CXU] * ey8 + K[CYU] * ex128
        p2 = p2 + K[PXU] * ey8
        p3 = p3 + K[PYU] * ex128
        hy_m = row_of(rxu, n, 0, z) + K[CXD] * ez
        hz_m = row_of(rxu, n, 1, z) - K[CXD] * ey + K[CYU] * roll_l(ca, 127 - z)
        hx_w = roll_l(yu, lax.rem(128 - z, 128)) - K[CYD] * ez
        hz_w = roll_l(yu, 64 - z) + K[CYD] * ex
        hz_dy = hz - jnp.where(l0, hz_w, roll_l(hz, 1))
        hx_dy = hx - jnp.where(l0, hx_w, roll_l(hx, 1))
        hz_dx = hz - jnp.where(s0, hz_m, roll_s(hz, 1))
        hy_dx = hy - jnp.where(s0, hy_m, roll_s(hy, 1))
        hy_dz = hy - hy_prev
        hx_dz = hx - hx_prev
        q0 = K[EDY] * PSI[4, z] + K[EGY] * hz_dy
        q1 = K[EDX] * PSI[5, z] + K[EGX] * hz_dx
        q2 = K[EDX] * PSI[6, z] + K[EGX] * hy_dx
        q3 = K[EDY] * PSI[7, z] + K[EGY] * hx_dy
        PSI[4, z], PSI[5, z], PSI[6, z], PSI[7, z] = q0, q1, q2, q3
        ce = CE[z]
        ex = ex + ce * (hz_dy + q0 - hy_dz)
        ey = ey + ce * (hx_dz - hz_dx - q1)
        ez = ez + ce * (hy_dx + q2 - hx_dy - q3)
        F[0, z], F[1, z], F[2, z] = ex, ey, ez
        return (ex, ey, ez), (hx, hy, hz), (p0, p1, p2, p3)

    def messages(n):
        def send(flag, i, src, dst, device):
            copy = pltpu.make_async_remote_copy(
                src_ref=src.at[n], dst_ref=dst.at[n],
                send_sem=hs_sem.at[n, i], recv_sem=hr_sem.at[n, i],
                device_id=device, device_id_type=MESH,
            )
            return flag, copy

        sends = [
            send(dn_x, 0, sxd, rxd, (row - 1, col)),
            send(up_x, 1, sxu, rxu, (row + 1, col)),
            send(dn_y, 2, syd, ryd, (row, col - 1)),
            send(up_y, 3, syu, ryu, (row, col + 1)),
            send(ca_out, 4, syd, rca, (row + 1, col - 1)),
            send(ca_in, 5, scb, rcb, (row - 1, col + 1)),
        ]
        arrives = [up_x, dn_x, up_y, dn_y, ca_in, ca_out]
        return sends, arrives

    def start_sends(n):
        for flag, copy in messages(n)[0]:
            pl.when(flag)(copy.start)

    def wait_arrivals(n):
        sends, arrives = messages(n)
        for (_, copy), flag in zip(sends, arrives):
            pl.when(flag)(copy.wait_recv)

    def wait_sends(n):
        for flag, copy in messages(n)[0]:
            pl.when(flag)(copy.wait_send)

    def mode_copy(j):
        dest = lax.rem(row + j, n_row)
        return pltpu.make_async_remote_copy(
            src_ref=basis.at[:, pl.ds(pl.multiple_of(dest * 8, 8), 8), :],
            dst_ref=W.at[pl.ds(row * modes_here, modes_here)],
            send_sem=bs_sem.at[j], recv_sem=br_sem.at[j],
            device_id=(dest, col), device_id_type=MESH,
        )

    def looped(first, last, step, carry):
        return lax.fori_loop(
            0, (last - first) // unroll,
            lambda i, c: functools.reduce(
                lambda c, u: step(first + i * unroll + u, c), range(unroll), c
            ),
            carry,
        )

    for copy in loads:
        copy.wait()

    def fields(base, z):
        return F[base, z], F[base + 1, z], F[base + 2, z]

    psi_zero = (zero,) * 4

    def opening(z, carry):
        E, (pd, pb, pu) = carry
        ahead = fields(0, z)
        pd, pb = pack_e(0, z, ahead, pd, pb)
        pu = finish_h(0, z - 1, E, fields(3, z - 1), psi_zero, ahead[0], ahead[1], pu)
        return ahead, (pd, pb, pu)

    first = fields(0, 0)
    pd, pb = pack_e(0, 0, first, zero, zero)
    last, (pd, pb, pu) = looped(1, nz, opening, (first, (pd, pb, zero)))
    pu = finish_h(0, nz - 1, last, fields(3, nz - 1), psi_zero, zero, zero, pu)
    syd[0], scb[0], syu[0] = pd, pb, pu
    pl.semaphore_wait(barrier, greeted)
    start_sends(0)

    def arrived(n):
        wait_arrivals(n)
        ca = jnp.broadcast_to(rca[n, 7:8, :], TILE)
        yu = ryu[n] - K[CXU] * jnp.broadcast_to(rcb[n, 0:1, :], TILE)
        return ryd[n], yu, ca

    @pl.loop(0, STEPS - 1)
    def _(n):
        @pl.when(n < n_row - 1)
        def _():
            mode_copy(n + 1).start()

        yd, yu, ca = arrived(n)

        def body(z, carry):
            E, H, psi, (pd, pb, pu) = carry
            E2, H2, psi2 = electric(n, z, yd, yu, ca, H[0], H[1])
            pd, pb = pack_e(n + 1, z, E2, pd, pb)
            pu = finish_h(n + 1, z - 1, E, H, psi, E2[0], E2[1], pu)
            return E2, H2, psi2, (pd, pb, pu)

        E, H, psi = electric(n, 0, yd, yu, ca, zero, zero)
        pd, pb = pack_e(n + 1, 0, E, zero, zero)
        E, H, psi, (pd, pb, pu) = looped(1, nz, body, (E, H, psi, (pd, pb, zero)))
        pu = finish_h(n + 1, nz - 1, E, H, psi, zero, zero, pu)
        syd[n + 1], scb[n + 1], syu[n + 1] = pd, pb, pu
        start_sends(n + 1)

    yd, yu, ca = arrived(STEPS - 1)

    def closing(z, carry):
        _, H, _ = electric(STEPS - 1, z, yd, yu, ca, carry[0], carry[1])
        F[3, z], F[4, z], F[5, z] = H
        return H[0], H[1]

    carry = closing(0, (zero, zero))
    looped(1, nz, closing, carry)

    stores = [
        pltpu.make_async_copy(F.at[0:3], e_out, out_sem.at[0]),
        pltpu.make_async_copy(F.at[3:6], h_out, out_sem.at[1]),
    ]
    for copy in stores:
        copy.start()

    count = snap.shape[0]
    rank = modes_here * n_row

    @pl.loop(0, count)
    def _(s):
        plane = snap[s]
        W[rank + s] = F[lax.div(plane, nz), lax.rem(plane, nz)]

    own_modes().wait()

    @pl.loop(1, n_row)
    def _(j):
        mode_copy(j).wait_recv()

    both = jnp.zeros((count, rank + count), f32)
    for x in range(8):
        both = both + lax.dot_general(
            W[rank:rank + count, x, :], W[:, x, :], (((1,), (1,)), ((), ())),
            precision=lax.Precision.HIGHEST, preferred_element_type=f32,
        )
    R[0:8] = both[:, :rank].reshape(8, 8, 128)
    gram = both[:, rank:] * (1.0 / (full_x * full_y))
    gram = jnp.concatenate([gram, jnp.zeros((count, 128 - count), f32)], axis=1)
    R[8:16] = gram.reshape(8, 8, 128)

    piece = 16 // n_a
    RA[a_me] = R[pl.ds(a_me * piece, piece)]

    def scatter(j):
        m = lax.rem(a_me + j, n_a)
        return pltpu.make_async_remote_copy(
            src_ref=R.at[pl.ds(m * piece, piece)], dst_ref=RA.at[a_me],
            send_sem=as_sem.at[j], recv_sem=ar_sem.at[j],
            device_id=a_device(m), device_id_type=MESH,
        )

    def exchange(j):
        m = lax.rem(b_me + j, n_b)
        return pltpu.make_async_remote_copy(
            src_ref=PB.at[b_me], dst_ref=PB.at[b_me],
            send_sem=ps_sem.at[j], recv_sem=pr_sem.at[j],
            device_id=b_device(m), device_id_type=MESH,
        )

    def gather(j):
        m = lax.rem(a_me + j, n_a)
        return pltpu.make_async_remote_copy(
            src_ref=G.at[a_me], dst_ref=G.at[a_me],
            send_sem=gs_sem.at[j], recv_sem=gr_sem.at[j],
            device_id=a_device(m), device_id_type=MESH,
        )

    def run(make, n):
        @pl.loop(1, n)
        def _(j):
            make(j).start()

        @pl.loop(1, n)
        def _(j):
            make(j).wait_recv()

    def total(ref, n):
        out = ref[0]
        for m in range(1, n):
            out = out + ref[m]
        return out

    run(scatter, n_a)
    PB[b_me] = total(RA, n_a)
    run(exchange, n_b)
    G[a_me] = total(PB, n_b)
    run(gather, n_a)
    whole = G[...].reshape(16, 8, 128)
    coef_out[...] = whole[0:8].reshape(64, 128)
    gram_out[...] = whole[8:16].reshape(64, 128)[:, :64]

    for copy in stores:
        copy.wait()

    @pl.loop(0, STEPS)
    def _(n):
        wait_sends(n)

    @pl.loop(1, n_row)
    def _(j):
        mode_copy(j).wait_send()

    @pl.loop(1, n_a)
    def _(j):
        scatter(j).wait_send()
        gather(j).wait_send()

    @pl.loop(1, n_b)
    def _(j):
        exchange(j).wait_send()


def solution(mesh):
    n_row, n_col = mesh.shape["row"], mesh.shape["col"]
    n_a, n_b = n_row * 2, n_col // 2
    piece = 16 // n_a

    def shards(e_field, h_field, e_coef, basis, pml_width, snap_index):
        nz = e_coef.shape[0]
        rank = basis.shape[0] * n_row
        count = snap_index.shape[0]
        dma = pltpu.SemaphoreType.DMA
        hbm = pl.BlockSpec(memory_space=pl.ANY)
        smem = pl.BlockSpec(memory_space=pltpu.SMEM)
        vmem = pl.BlockSpec(memory_space=pltpu.VMEM)
        planes = pltpu.VMEM((STEPS, 2, nz, 128), f32)
        tiles = pltpu.VMEM((STEPS, 8, 128), f32)
        return pl.pallas_call(
            functools.partial(kernel, n_row, n_col, nz, 3 if nz == 64 else 1),
            out_shape=(
                jax.ShapeDtypeStruct(e_field.shape, f32),
                jax.ShapeDtypeStruct(h_field.shape, f32),
                jax.ShapeDtypeStruct((count, rank), f32),
                jax.ShapeDtypeStruct((count, count), f32),
            ),
            in_specs=[hbm, hbm, hbm, hbm, smem, smem],
            out_specs=(hbm, hbm, vmem, vmem),
            scratch_shapes=[
                pltpu.VMEM((6, nz, 8, 128), f32),
                pltpu.VMEM((nz, 8, 128), f32),
                pltpu.VMEM((8, nz, 8, 128), f32),
                pltpu.VMEM((14, 8, 128), f32),
                planes, planes, tiles, tiles, tiles,
                planes, planes, tiles, tiles, tiles, tiles,
                pltpu.VMEM((rank + count, 8, 128), f32),
                pltpu.VMEM((16, 8, 128), f32),
                pltpu.VMEM((n_a, piece, 8, 128), f32),
                pltpu.VMEM((n_b, piece, 8, 128), f32),
                pltpu.VMEM((n_a, piece, 8, 128), f32),
                dma((3,)), dma((2,)), dma((STEPS, 6)), dma((STEPS, 6)),
                dma((n_row,)), dma((n_row,)), dma((1,)),
                dma((n_a,)), dma((n_a,)), dma((n_b,)), dma((n_b,)), dma((n_a,)), dma((n_a,)),
            ],
            compiler_params=pltpu.CompilerParams(collective_id=0, has_side_effects=True),
            name="yee",
        )(e_field, h_field, e_coef, basis, pml_width, snap_index)

    return jax.shard_map(
        shards,
        mesh=mesh,
        in_specs=(
            P(None, None, "row", "col"),
            P(None, None, "row", "col"),
            P(None, "row", "col"),
            P("row", None, "col"),
            P(),
            P(),
        ),
        out_specs=(P(None, None, "row", "col"), P(None, None, "row", "col"), P(), P()),
        check_vma=False,
    )
```

```python
import functools

import jax
import jax.numpy as jnp
from jax import lax
from jax.experimental import pallas as pl
from jax.experimental.pallas import tpu as pltpu
from jax.sharding import PartitionSpec as P

STEPS = 8
time_step = 0.5
sigma_top = 4.0
alpha_shift = 0.05
MESH = pl.DeviceIdType.MESH
TILE = (8, 128)
f32 = jnp.float32


def absorber(positions, total, low, high):
    depth = jnp.maximum(
        jnp.maximum((low - positions) / low, (positions - (total - 1.0 - high)) / high), 0.0
    )
    sigma = sigma_top * (depth * depth * depth)
    damp = jnp.exp(-(sigma + alpha_shift) * time_step)
    gain = sigma / (sigma + alpha_shift) * (damp - 1.0)
    return damp, gain


def kernel(
    n_row, n_col, nz, chunks,
    e_in, h_in, c_in, basis, pml, snap,
    e_out, h_out, coef_out, gram_out,
    F, CE, HP, PSIH, PSIE, K, CAR,
    sxd, sxu, syd, syu, sca, scb,
    rxd, rxu, ryd, ryu, rca, rcb,
    W, M, R, RA, PB, G,
    in_sem, out_sem, hs_sem, hr_sem, bs_sem, br_sem, own_sem,
    as_sem, ar_sem, ps_sem, pr_sem, gs_sem, gr_sem,
):
    pad = STEPS
    deep = -(-(nz + pad) // chunks)
    tall = F.shape[1]
    row = lax.axis_index("row")
    col = lax.axis_index("col")
    n_a, n_b = n_row * 2, n_col // 2
    y_lo = lax.rem(lax.div(col, 2), 2)
    a_me = row * 2 + y_lo
    b_me = lax.div(col, 4) * 2 + lax.rem(col, 2)

    def a_device(m):
        return (lax.div(m, 2), lax.div(col, 4) * 4 + lax.rem(m, 2) * 2 + lax.rem(col, 2))

    def b_device(m):
        return (row, lax.div(m, 2) * 4 + y_lo * 2 + lax.rem(m, 2))

    loads = [
        pltpu.make_async_copy(e_in, F.at[0:3, pad:pad + nz], in_sem.at[0]),
        pltpu.make_async_copy(h_in, F.at[3:6, pad:pad + nz], in_sem.at[1]),
        pltpu.make_async_copy(c_in, CE.at[pad:pad + nz], in_sem.at[2]),
    ]
    for copy in loads:
        copy.start()
    modes_here = basis.shape[0]

    def modes_for(dest):
        return pltpu.make_async_copy(basis.at[:, 8 * dest:8 * dest + 8, :], M.at[dest], own_sem.at[0])

    for dest in range(n_row):
        modes_for(dest).start()

    barrier = pltpu.get_barrier_semaphore()

    def greet(device):
        pl.semaphore_signal(barrier, inc=1, device_id=device, device_id_type=MESH)

    @pl.loop(1, n_a)
    def _(j):
        greet(a_device(lax.rem(a_me + j, n_a)))

    @pl.loop(1, n_b)
    def _(j):
        greet(b_device(lax.rem(b_me + j, n_b)))

    up_x, dn_x = row < n_row - 1, row > 0
    up_y, dn_y = col < n_col - 1, col > 0
    ca_out, ca_in = up_x & dn_y, dn_x & up_y

    @pl.when(up_y)
    def _():
        greet((row, col + 1))

    @pl.when(dn_y)
    def _():
        greet((row, col - 1))

    @pl.when(ca_out)
    def _():
        greet((row + 1, col - 1))

    @pl.when(ca_in)
    def _():
        greet((row - 1, col + 1))

    greeted = n_a - 1 + n_b - 1
    for flag in (up_y, dn_y, ca_out, ca_in):
        greeted = greeted + flag.astype(jnp.int32)

    sub = lax.broadcasted_iota(jnp.int32, TILE, 0)
    lane = lax.broadcasted_iota(jnp.int32, TILE, 1)
    w = [jnp.full(TILE, pml[i], jnp.int32).astype(f32) for i in range(4)]
    x_pos = (row * 8 + sub).astype(f32)
    y_pos = (col * 128 + lane).astype(f32)
    full_x, full_y = float(n_row * 8), float(n_col * 128)
    hdx, hgx = absorber(x_pos + 0.5, full_x, w[0], w[1])
    hdy, hgy = absorber(y_pos + 0.5, full_y, w[2], w[3])
    edx, egx = absorber(x_pos, full_x, w[0], w[1])
    edy, egy = absorber(y_pos, full_y, w[2], w[3])
    _, gxm = absorber((row * 8 - 1 + 0 * sub).astype(f32) + 0.5, full_x, w[0], w[1])
    _, gym = absorber((col * 128 - 1 + 0 * lane).astype(f32) + 0.5, full_y, w[2], w[3])
    s7, s0, l127, l0 = sub == 7, sub == 0, lane == 127, lane == 0
    zero = jnp.zeros(TILE, f32)
    coeffs = [
        hdx, hgx, hdy, hgy, edx, egx, edy, egy,
        jnp.where(s7, 0.5 * (1.0 + hgx), zero), jnp.where(s7, hgx, zero),
        jnp.where(l127, 0.5 * (1.0 + hgy), zero), jnp.where(l127, hgy, zero),
        0.5 * (1.0 + gxm) * dn_x.astype(f32), 0.5 * (1.0 + gym) * dn_y.astype(f32),
    ]
    for i, value in enumerate(coeffs):
        K[i] = value
    HDX, HGX, HDY, HGY, EDX, EGX, EDY, EGY, CXU, PXU, CYU, PYU, CXD, CYD = range(14)

    @pl.loop(0, tall)
    def _(z):
        for i in range(4):
            PSIE[i, z] = zero
            PSIH[i, z] = zero

    for beyond in (*range(pad), *range(pad + nz, tall)):
        CE[beyond] = zero
        for i in range(6):
            F[i, beyond] = zero

    def clear(ref, wanted):
        @pl.when(wanted)
        def _():
            @pl.loop(0, STEPS)
            def _(n):
                ref[n] = jnp.zeros(ref.shape[1:], f32)

    clear(rxd, ~up_x)
    clear(rxu, ~dn_x)
    clear(ryd, ~up_y)
    clear(ryu, ~dn_y)
    clear(rca, ~ca_in)
    clear(rcb, ~ca_out)

    def wide(v):
        return jnp.broadcast_to(v, TILE)

    def roll_l(v, by):
        by = by % 128
        return pltpu.roll(v, by, 1) if by else v

    def roll_s(v, by):
        return pltpu.roll(v, by, 0)

    def partial_h(E, H, psi, ex_next, ey_next):
        ex, ey, ez = E
        hx, hy, hz = H
        ez_dy = jnp.where(l127, 0.0, roll_l(ez, 127)) - ez
        ex_dy = jnp.where(l127, 0.0, roll_l(ex, 127)) - ex
        ez_dx = jnp.where(s7, 0.0, roll_s(ez, 7)) - ez
        ey_dx = jnp.where(s7, 0.0, roll_s(ey, 7)) - ey
        ey_dz = ey_next - ey
        ex_dz = ex_next - ex
        p0, p1, p2, p3 = K[HGY] * ez_dy, K[HGX] * ez_dx, K[HGX] * ey_dx, K[HGY] * ex_dy
        if psi is not None:
            p0, p1 = K[HDY] * psi[0] + p0, K[HDX] * psi[1] + p1
            p2, p3 = K[HDX] * psi[2] + p2, K[HDY] * psi[3] + p3
        hx = hx - time_step * (ez_dy + p0 - ey_dz)
        hy = hy - time_step * (ex_dz - ez_dx - p1)
        hz = hz - time_step * (ey_dx + p2 - ex_dy - p3)
        return (hx, hy, hz), (p0, p1, p2, p3)

    def put(packed, i, low, high):
        if low is not None:
            packed = jnp.where(lane == i, low, packed)
        return jnp.where(lane == 64 + i, high, packed)

    def pack_e(n, c, i, E, pd):
        ex, ey, ez = E
        sxd[n, c, 2 * i:2 * i + 1, :] = ey[0:1, :]
        sxd[n, c, 2 * i + 1:2 * i + 2, :] = ez[0:1, :]
        return put(pd, i, roll_l(ex, i), roll_l(ez, 64 + i))

    def finish_h(n, c, i, z, E, H, later, ex_next, ey_next, pu, pb):
        psi = tuple(PSIH[k, z + pad] for k in range(4)) if later else None
        H, psi = partial_h(E, H, psi, ex_next, ey_next)
        for k in range(3):
            HP[k, z + pad] = H[k]
        for k in range(4):
            PSIH[k, z + pad] = psi[k]
        sxu[n, c, 2 * i:2 * i + 1, :] = H[1][7:8, :]
        sxu[n, c, 2 * i + 1:2 * i + 2, :] = H[2][7:8, :]
        pu = put(pu, i, roll_l(H[0], i - 127), roll_l(H[2], 64 + i - 127))
        pb = put(pb, i, None, roll_l(E[1], 64 + i - 127))
        return pu, pb

    def electric(n, c, i, z, yds, yu, cas, hx_prev, hy_prev):
        p = z + pad
        ex, ey, ez = F[0, p], F[1, p], F[2, p]
        hx, hy, hz = HP[0, p], HP[1, p], HP[2, p]
        p0, p1, p2, p3 = PSIH[0, p], PSIH[1, p], PSIH[2, p], PSIH[3, p]
        if i == 0:
            k, j = lax.max(c - 1, 0), deep - 1
        else:
            k, j = c, i - 1
        yd, ca = yds[i > 0], cas[i > 0]
        ey8 = wide(rxd[n, k, 2 * j:2 * j + 1, :])
        ez8 = wide(rxd[n, k, 2 * j + 1:2 * j + 2, :])
        ex128, ez128 = roll_l(yd, 127 - j), roll_l(yd, 63 - j)
        if i <= pad:
            hx_prev = jnp.where(z == 0, zero, hx_prev)
            hy_prev = jnp.where(z == 0, zero, hy_prev)
        hy = hy + K[CXU] * ez8
        p1 = p1 + K[PXU] * ez8
        hx = hx - K[CYU] * ez128
        p0 = p0 + K[PYU] * ez128
        hz = hz - K[CXU] * ey8 + K[CYU] * ex128
        p2 = p2 + K[PXU] * ey8
        p3 = p3 + K[PYU] * ex128
        hy_m = wide(rxu[n, c, 2 * i:2 * i + 1, :]) + K[CXD] * ez
        hz_m = wide(rxu[n, c, 2 * i + 1:2 * i + 2, :]) - K[CXD] * ey
        hz_m = hz_m + K[CYU] * roll_l(ca, 127 - j)
        hx_w = roll_l(yu, -i) - K[CYD] * ez
        hz_w = roll_l(yu, 64 - i) + K[CYD] * ex
        hz_dy = hz - jnp.where(l0, hz_w, roll_l(hz, 1))
        hx_dy = hx - jnp.where(l0, hx_w, roll_l(hx, 1))
        hz_dx = hz - jnp.where(s0, hz_m, roll_s(hz, 1))
        hy_dx = hy - jnp.where(s0, hy_m, roll_s(hy, 1))
        hy_dz = hy - hy_prev
        hx_dz = hx - hx_prev
        q0 = K[EDY] * PSIE[0, p] + K[EGY] * hz_dy
        q1 = K[EDX] * PSIE[1, p] + K[EGX] * hz_dx
        q2 = K[EDX] * PSIE[2, p] + K[EGX] * hy_dx
        q3 = K[EDY] * PSIE[3, p] + K[EGY] * hx_dy
        PSIE[0, p], PSIE[1, p], PSIE[2, p], PSIE[3, p] = q0, q1, q2, q3
        ce = CE[p]
        ex = ex + ce * (hz_dy + q0 - hy_dz)
        ey = ey + ce * (hx_dz - hz_dx - q1)
        ez = ez + ce * (hy_dx + q2 - hx_dy - q3)
        F[0, p], F[1, p], F[2, p] = ex, ey, ez
        PSIH[0, p], PSIH[1, p], PSIH[2, p], PSIH[3, p] = p0, p1, p2, p3
        return (ex, ey, ez), (hx, hy, hz)

    routes = [
        (dn_x, up_x, sxd, rxd, (row - 1, col)),
        (up_x, dn_x, sxu, rxu, (row + 1, col)),
        (dn_y, up_y, syd, ryd, (row, col - 1)),
        (up_y, dn_y, syu, ryu, (row, col + 1)),
        (ca_out, ca_in, sca, rca, (row + 1, col - 1)),
        (ca_in, ca_out, scb, rcb, (row - 1, col + 1)),
    ]

    def message(i, n, c):
        _, _, src, dst, device = routes[i]
        return pltpu.make_async_remote_copy(
            src_ref=src.at[n, c], dst_ref=dst.at[n, c],
            send_sem=hs_sem.at[i], recv_sem=hr_sem.at[lax.rem(n, 2), c, i],
            device_id=device, device_id_type=MESH,
        )

    def arrived(n, c):
        for i in range(6):
            pl.when(routes[i][1])(lambda: message(i, n, c).wait_recv())
        before = lax.max(c - 1, 0)
        yu = ryu[n, c] - K[CXU] * wide(rcb[n, c])
        cas = wide(rca[n, before]), wide(rca[n, c])
        return (ryd[n, before], ryd[n, c]), yu, cas

    def send(n, c, pd, pu, pb):
        syd[n, c], syu[n, c], sca[n, c], scb[n, c] = pd, pu, pd[7:8, :], pb[0:1, :]
        for i in (4, 5, 0, 1, 2, 3):
            pl.when(routes[i][0])(lambda: message(i, n, c).start())

    def bytes_of(ref, sem):
        pltpu.make_async_copy(ref, ref, sem).wait()

    def all_left():
        for i in range(6):
            pl.when(routes[i][0])(lambda: bytes_of(routes[i][2], hs_sem.at[i]))

    def mode_copy(j, first, count):
        dest = lax.rem(row + j, n_row)
        return pltpu.make_async_remote_copy(
            src_ref=M.at[dest, pl.ds(first, count)],
            dst_ref=W.at[pl.ds(row * modes_here + first, count)],
            send_sem=bs_sem.at[0], recv_sem=br_sem.at[0],
            device_id=(dest, col), device_id_type=MESH,
        )

    def mode_piece(k):
        half = modes_here // 2
        mode_copy(1 + 2 * lax.div(k, 2), lax.rem(k, 2) * half, half).start()

    for copy in loads:
        copy.wait()
    pl.semaphore_wait(barrier, greeted)
    none = (zero, zero, zero)

    def opening(c, carry):
        E, H = carry
        pd = pu = pb = zero
        for i in range(deep):
            z = c * deep + i
            p = z + pad
            ahead = F[0, p], F[1, p], F[2, p]
            pd = pack_e(0, c, i, ahead, pd)
            pu, pb = finish_h(0, c, i, z - 1, E, H, False, ahead[0], ahead[1], pu, pb)
            E, H = ahead, (F[3, p], F[4, p], F[5, p])
        send(0, c, pd, pu, pb)
        return E, H

    lax.fori_loop(0, chunks, opening, (none, none))
    for k in range(3):
        CAR[k] = zero
    bytes_of(M, own_sem.at[0])
    for j in range(2, n_row, 2):
        mode_copy(j, 0, modes_here).start()
    mode_piece(n_row - 1)

    @pl.loop(0, STEPS - 1)
    def _(n):
        @pl.when(n < n_row - 1)
        def _():
            mode_piece(n)

        @pl.loop(0, chunks)
        def _(c):
            yds, yu, cas = arrived(n, c)
            pd = pu = pb = zero
            below = c * deep - (n + 2) + pad
            E = F[0, below], F[1, below], F[2, below]
            H = CAR[0], CAR[1], CAR[2]
            for i in range(deep):
                z = c * deep - (n + 1) + i
                E2, H2 = electric(n, c, i, z, yds, yu, cas, H[0], H[1])
                pd = pack_e(n + 1, c, i, E2, pd)
                pu, pb = finish_h(n + 1, c, i, z - 1, E, H, True, E2[0], E2[1], pu, pb)
                E, H = E2, H2
            for k, value in enumerate(H):
                CAR[k] = value
            send(n + 1, c, pd, pu, pb)

    def closing(c, carry):
        n = STEPS - 1
        yds, yu, cas = arrived(n, c)
        for i in range(deep):
            z = c * deep - (n + 1) + i
            _, H = electric(n, c, i, z, yds, yu, cas, carry[0], carry[1])
            F[3, z + pad], F[4, z + pad], F[5, z + pad] = H
            carry = H[0], H[1]
        return carry

    lax.fori_loop(0, chunks, closing, (zero, zero))

    stores = [
        pltpu.make_async_copy(F.at[0:3, pad:pad + nz], e_out, out_sem.at[0]),
        pltpu.make_async_copy(F.at[3:6, pad:pad + nz], h_out, out_sem.at[1]),
    ]
    for copy in stores:
        copy.start()

    count = snap.shape[0]
    rank = modes_here * n_row

    @pl.loop(0, count // 8)
    def _(g):
        for k in range(8):
            plane = snap[g * 8 + k]
            W[rank + g * 8 + k] = F[lax.div(plane, nz), pad + lax.rem(plane, nz)]

    W[pl.ds(row * modes_here, modes_here)] = M[row]

    elsewhere = W.at[0:rank - modes_here]
    bytes_of(elsewhere, br_sem.at[0])

    both = jnp.zeros((count, rank + count), f32)
    for x in range(8):
        both = both + lax.dot_general(
            W[rank:rank + count, x, :], W[:, x, :], (((1,), (1,)), ((), ())),
            precision=lax.Precision.HIGHEST, preferred_element_type=f32,
        )
    R[0:8] = both[:, :rank].reshape(8, 8, 128)
    gram = both[:, rank:] * (1.0 / (full_x * full_y))
    gram = jnp.concatenate([gram, jnp.zeros((count, 128 - count), f32)], axis=1)
    R[8:16] = gram.reshape(8, 8, 128)

    piece = 16 // n_a
    RA[a_me] = R[pl.ds(a_me * piece, piece)]

    def scatter(j):
        m = lax.rem(a_me + j, n_a)
        return pltpu.make_async_remote_copy(
            src_ref=R.at[pl.ds(m * piece, piece)], dst_ref=RA.at[a_me],
            send_sem=as_sem.at[0], recv_sem=ar_sem.at[0],
            device_id=a_device(m), device_id_type=MESH,
        )

    def exchange(j):
        m = lax.rem(b_me + j, n_b)
        return pltpu.make_async_remote_copy(
            src_ref=PB.at[b_me], dst_ref=PB.at[b_me],
            send_sem=ps_sem.at[0], recv_sem=pr_sem.at[0],
            device_id=b_device(m), device_id_type=MESH,
        )

    def gather(j):
        m = lax.rem(a_me + j, n_a)
        return pltpu.make_async_remote_copy(
            src_ref=G.at[a_me], dst_ref=G.at[a_me],
            send_sem=gs_sem.at[0], recv_sem=gr_sem.at[0],
            device_id=a_device(m), device_id_type=MESH,
        )

    def run(make, n, land, sem, meanwhile=None):
        @pl.loop(1, n)
        def _(j):
            make(j).start()

        if meanwhile is not None:
            meanwhile()
        bytes_of(land.at[0:n - 1], sem.at[0])

    def total(ref, n):
        out = ref[0]
        for m in range(1, n):
            out = out + ref[m]
        return out

    run(scatter, n_a, RA, ar_sem, all_left)
    PB[b_me] = total(RA, n_a)
    run(exchange, n_b, PB, pr_sem)
    G[a_me] = total(PB, n_b)
    run(gather, n_a, G, gr_sem)
    whole = G[...].reshape(16, 8, 128)
    coef_out[...] = whole[0:8].reshape(64, 128)
    gram_out[...] = whole[8:16].reshape(64, 128)[:, :64]

    for copy in stores:
        copy.wait()

    bytes_of(elsewhere, bs_sem.at[0])
    bytes_of(RA.at[0:n_a - 1], as_sem.at[0])
    bytes_of(PB.at[0:n_b - 1], ps_sem.at[0])
    bytes_of(G.at[0:n_a - 1], gs_sem.at[0])


def solution(mesh):
    n_row, n_col = mesh.shape["row"], mesh.shape["col"]
    n_a, n_b = n_row * 2, n_col // 2
    piece = 16 // n_a

    def shards(e_field, h_field, e_coef, basis, pml_width, snap_index):
        nz = e_coef.shape[0]
        rank = basis.shape[0] * n_row
        count = snap_index.shape[0]
        dma = pltpu.SemaphoreType.DMA
        hbm = pl.BlockSpec(memory_space=pl.ANY)
        smem = pl.BlockSpec(memory_space=pltpu.SMEM)
        vmem = pl.BlockSpec(memory_space=pltpu.VMEM)
        chunks = 6 if nz == 64 else 2
        deep = -(-(nz + STEPS) // chunks)
        tall = deep * chunks + STEPS
        rows = pltpu.VMEM((STEPS, chunks, -(-deep // 4) * 8, 128), f32)
        tiles = pltpu.VMEM((STEPS, chunks, 8, 128), f32)
        lines = pltpu.VMEM((STEPS, chunks, 1, 128), f32)
        return pl.pallas_call(
            functools.partial(kernel, n_row, n_col, nz, chunks),
            out_shape=(
                jax.ShapeDtypeStruct(e_field.shape, f32),
                jax.ShapeDtypeStruct(h_field.shape, f32),
                jax.ShapeDtypeStruct((count, rank), f32),
                jax.ShapeDtypeStruct((count, count), f32),
            ),
            in_specs=[hbm, hbm, hbm, hbm, smem, smem],
            out_specs=(hbm, hbm, vmem, vmem),
            scratch_shapes=[
                pltpu.VMEM((6, tall, 8, 128), f32),
                pltpu.VMEM((tall, 8, 128), f32),
                pltpu.VMEM((3, tall, 8, 128), f32),
                pltpu.VMEM((4, tall, 8, 128), f32),
                pltpu.VMEM((4, tall, 8, 128), f32),
                pltpu.VMEM((14, 8, 128), f32),
                pltpu.VMEM((3, 8, 128), f32),
                rows, rows, tiles, tiles, lines, lines,
                rows, rows, tiles, tiles, lines, lines,
                pltpu.VMEM((rank + count, 8, 128), f32),
                pltpu.VMEM((n_row, basis.shape[0], 8, 128), f32),
                pltpu.VMEM((16, 8, 128), f32),
                pltpu.VMEM((n_a, piece, 8, 128), f32),
                pltpu.VMEM((n_b, piece, 8, 128), f32),
                pltpu.VMEM((n_a, piece, 8, 128), f32),
                dma((3,)), dma((2,)), dma((6,)), dma((2, chunks, 6)),
                dma((1,)), dma((1,)), dma((1,)),
                dma((1,)), dma((1,)), dma((1,)), dma((1,)), dma((1,)), dma((1,)),
            ],
            compiler_params=pltpu.CompilerParams(collective_id=0, has_side_effects=True),
            name="yee",
        )(e_field, h_field, e_coef, basis, pml_width, snap_index)

    return jax.shard_map(
        shards,
        mesh=mesh,
        in_specs=(
            P(None, None, "row", "col"),
            P(None, None, "row", "col"),
            P(None, "row", "col"),
            P("row", None, "col"),
            P(),
            P(),
        ),
        out_specs=(P(None, None, "row", "col"), P(None, None, "row", "col"), P(), P()),
        check_vma=False,
    )
```

```python
import functools

import jax
import jax.numpy as jnp
from jax import lax
from jax.experimental import pallas as pl
from jax.experimental.pallas import tpu as pltpu
from jax.sharding import PartitionSpec as P

STEPS = 8
time_step = 0.5
sigma_top = 4.0
alpha_shift = 0.05
MESH = pl.DeviceIdType.MESH
TILE = (8, 128)
f32 = jnp.float32


def absorber(positions, total, low, high):
    depth = jnp.maximum(
        jnp.maximum((low - positions) / low, (positions - (total - 1.0 - high)) / high), 0.0
    )
    sigma = sigma_top * (depth * depth * depth)
    damp = jnp.exp(-(sigma + alpha_shift) * time_step)
    gain = sigma / (sigma + alpha_shift) * (damp - 1.0)
    return damp, gain


def kernel(
    n_row, n_col, nz, chunks,
    e_in, h_in, c_in, basis, pml, snap,
    F, coef_out, gram_out,
    CE, HP, PSIH, PSIE, K, CAR,
    sxd, sxu, syd, syu, sca, scb,
    rxd, rxu, ryd, ryu, rca, rcb,
    W, M, R, RA, PB, G,
    in_sem, hs_sem, hr_sem, bs_sem, br_sem, own_sem,
    as_sem, ar_sem, ps_sem, pr_sem, gs_sem, gr_sem,
):
    pad = STEPS
    deep = -(-(nz + pad) // chunks)
    tall = F.shape[1]
    row = lax.axis_index("row")
    col = lax.axis_index("col")
    n_a, n_b = n_row * 2, n_col // 2
    y_lo = lax.rem(lax.div(col, 2), 2)
    a_me = row * 2 + y_lo
    b_me = lax.div(col, 4) * 2 + lax.rem(col, 2)

    def a_device(m):
        return (lax.div(m, 2), lax.div(col, 4) * 4 + lax.rem(m, 2) * 2 + lax.rem(col, 2))

    def b_device(m):
        return (row, lax.div(m, 2) * 4 + y_lo * 2 + lax.rem(m, 2))

    loads = [
        pltpu.make_async_copy(e_in, F.at[0:3, pad:pad + nz], in_sem.at[0]),
        pltpu.make_async_copy(h_in, F.at[3:6, pad:pad + nz], in_sem.at[1]),
        pltpu.make_async_copy(c_in, CE.at[pad:pad + nz], in_sem.at[2]),
    ]
    for copy in loads:
        copy.start()
    modes_here = basis.shape[0]

    def modes_for(dest):
        return pltpu.make_async_copy(basis.at[:, 8 * dest:8 * dest + 8, :], M.at[dest], own_sem.at[0])

    for dest in range(n_row):
        modes_for(dest).start()

    barrier = pltpu.get_barrier_semaphore()

    def greet(device):
        pl.semaphore_signal(barrier, inc=1, device_id=device, device_id_type=MESH)

    @pl.loop(1, n_a)
    def _(j):
        greet(a_device(lax.rem(a_me + j, n_a)))

    @pl.loop(1, n_b)
    def _(j):
        greet(b_device(lax.rem(b_me + j, n_b)))

    up_x, dn_x = row < n_row - 1, row > 0
    up_y, dn_y = col < n_col - 1, col > 0
    ca_out, ca_in = up_x & dn_y, dn_x & up_y

    @pl.when(up_y)
    def _():
        greet((row, col + 1))

    @pl.when(dn_y)
    def _():
        greet((row, col - 1))

    @pl.when(ca_out)
    def _():
        greet((row + 1, col - 1))

    @pl.when(ca_in)
    def _():
        greet((row - 1, col + 1))

    greeted = n_a - 1 + n_b - 1
    for flag in (up_y, dn_y, ca_out, ca_in):
        greeted = greeted + flag.astype(jnp.int32)

    sub = lax.broadcasted_iota(jnp.int32, TILE, 0)
    lane = lax.broadcasted_iota(jnp.int32, TILE, 1)
    w = [jnp.full(TILE, pml[i], jnp.int32).astype(f32) for i in range(4)]
    x_pos = (row * 8 + sub).astype(f32)
    y_pos = (col * 128 + lane).astype(f32)
    full_x, full_y = float(n_row * 8), float(n_col * 128)
    hdx, hgx = absorber(x_pos + 0.5, full_x, w[0], w[1])
    hdy, hgy = absorber(y_pos + 0.5, full_y, w[2], w[3])
    edx, egx = absorber(x_pos, full_x, w[0], w[1])
    edy, egy = absorber(y_pos, full_y, w[2], w[3])
    _, gxm = absorber((row * 8 - 1 + 0 * sub).astype(f32) + 0.5, full_x, w[0], w[1])
    _, gym = absorber((col * 128 - 1 + 0 * lane).astype(f32) + 0.5, full_y, w[2], w[3])
    s7, s0, l127, l0 = sub == 7, sub == 0, lane == 127, lane == 0
    zero = jnp.zeros(TILE, f32)
    coeffs = [
        hdx, hgx, hdy, hgy, edx, egx, edy, egy,
        jnp.where(s7, 0.5 * (1.0 + hgx), zero), jnp.where(s7, hgx, zero),
        jnp.where(l127, 0.5 * (1.0 + hgy), zero), jnp.where(l127, hgy, zero),
        0.5 * (1.0 + gxm) * dn_x.astype(f32), 0.5 * (1.0 + gym) * dn_y.astype(f32),
    ]
    for i, value in enumerate(coeffs):
        K[i] = value
    HDX, HGX, HDY, HGY, EDX, EGX, EDY, EGY, CXU, PXU, CYU, PYU, CXD, CYD = range(14)

    @pl.loop(0, tall)
    def _(z):
        for i in range(4):
            PSIE[i, z] = zero
            PSIH[i, z] = zero

    for beyond in (*range(pad), *range(pad + nz, tall)):
        CE[beyond] = zero
        for i in range(6):
            F[i, beyond] = zero

    def clear(ref, wanted):
        @pl.when(wanted)
        def _():
            @pl.loop(0, STEPS)
            def _(n):
                ref[n] = jnp.zeros(ref.shape[1:], f32)

    clear(rxd, ~up_x)
    clear(rxu, ~dn_x)
    clear(ryd, ~up_y)
    clear(ryu, ~dn_y)
    clear(rca, ~ca_in)
    clear(rcb, ~ca_out)

    def wide(v):
        return jnp.broadcast_to(v, TILE)

    def roll_l(v, by):
        by = by % 128
        return pltpu.roll(v, by, 1) if by else v

    def roll_s(v, by):
        return pltpu.roll(v, by, 0)

    def partial_h(E, H, psi, ex_next, ey_next):
        ex, ey, ez = E
        hx, hy, hz = H
        ez_dy = jnp.where(l127, 0.0, roll_l(ez, 127)) - ez
        ex_dy = jnp.where(l127, 0.0, roll_l(ex, 127)) - ex
        ez_dx = jnp.where(s7, 0.0, roll_s(ez, 7)) - ez
        ey_dx = jnp.where(s7, 0.0, roll_s(ey, 7)) - ey
        ey_dz = ey_next - ey
        ex_dz = ex_next - ex
        p0, p1, p2, p3 = K[HGY] * ez_dy, K[HGX] * ez_dx, K[HGX] * ey_dx, K[HGY] * ex_dy
        if psi is not None:
            p0, p1 = K[HDY] * psi[0] + p0, K[HDX] * psi[1] + p1
            p2, p3 = K[HDX] * psi[2] + p2, K[HDY] * psi[3] + p3
        hx = hx - time_step * (ez_dy + p0 - ey_dz)
        hy = hy - time_step * (ex_dz - ez_dx - p1)
        hz = hz - time_step * (ey_dx + p2 - ex_dy - p3)
        return (hx, hy, hz), (p0, p1, p2, p3)

    def put(packed, i, low, high):
        if low is not None:
            packed = jnp.where(lane == i, low, packed)
        return jnp.where(lane == 64 + i, high, packed)

    def pack_e(n, c, i, E, pd):
        ex, ey, ez = E
        sxd[n, c, 2 * i:2 * i + 1, :] = ey[0:1, :]
        sxd[n, c, 2 * i + 1:2 * i + 2, :] = ez[0:1, :]
        return put(pd, i, roll_l(ex, i), roll_l(ez, 64 + i))

    def finish_h(n, c, i, z, E, H, later, ex_next, ey_next, pu, pb):
        psi = tuple(PSIH[k, z + pad] for k in range(4)) if later else None
        H, psi = partial_h(E, H, psi, ex_next, ey_next)
        for k in range(3):
            HP[k, z + pad] = H[k]
        for k in range(4):
            PSIH[k, z + pad] = psi[k]
        sxu[n, c, 2 * i:2 * i + 1, :] = H[1][7:8, :]
        sxu[n, c, 2 * i + 1:2 * i + 2, :] = H[2][7:8, :]
        pu = put(pu, i, roll_l(H[0], i - 127), roll_l(H[2], 64 + i - 127))
        pb = put(pb, i, None, roll_l(E[1], 64 + i - 127))
        return pu, pb

    def electric(n, c, i, z, yds, yu, cas, hx_prev, hy_prev):
        p = z + pad
        ex, ey, ez = F[0, p], F[1, p], F[2, p]
        hx, hy, hz = HP[0, p], HP[1, p], HP[2, p]
        p0, p1, p2, p3 = PSIH[0, p], PSIH[1, p], PSIH[2, p], PSIH[3, p]
        if i == 0:
            k, j = lax.max(c - 1, 0), deep - 1
        else:
            k, j = c, i - 1
        yd, ca = yds[i > 0], cas[i > 0]
        ey8 = wide(rxd[n, k, 2 * j:2 * j + 1, :])
        ez8 = wide(rxd[n, k, 2 * j + 1:2 * j + 2, :])
        ex128, ez128 = roll_l(yd, 127 - j), roll_l(yd, 63 - j)
        if i <= pad:
            hx_prev = jnp.where(z == 0, zero, hx_prev)
            hy_prev = jnp.where(z == 0, zero, hy_prev)
        hy = hy + K[CXU] * ez8
        p1 = p1 + K[PXU] * ez8
        hx = hx - K[CYU] * ez128
        p0 = p0 + K[PYU] * ez128
        hz = hz - K[CXU] * ey8 + K[CYU] * ex128
        p2 = p2 + K[PXU] * ey8
        p3 = p3 + K[PYU] * ex128
        hy_m = wide(rxu[n, c, 2 * i:2 * i + 1, :]) + K[CXD] * ez
        hz_m = wide(rxu[n, c, 2 * i + 1:2 * i + 2, :]) - K[CXD] * ey
        hz_m = hz_m + K[CYU] * roll_l(ca, 127 - j)
        hx_w = roll_l(yu, -i) - K[CYD] * ez
        hz_w = roll_l(yu, 64 - i) + K[CYD] * ex
        hz_dy = hz - jnp.where(l0, hz_w, roll_l(hz, 1))
        hx_dy = hx - jnp.where(l0, hx_w, roll_l(hx, 1))
        hz_dx = hz - jnp.where(s0, hz_m, roll_s(hz, 1))
        hy_dx = hy - jnp.where(s0, hy_m, roll_s(hy, 1))
        hy_dz = hy - hy_prev
        hx_dz = hx - hx_prev
        q0 = K[EDY] * PSIE[0, p] + K[EGY] * hz_dy
        q1 = K[EDX] * PSIE[1, p] + K[EGX] * hz_dx
        q2 = K[EDX] * PSIE[2, p] + K[EGX] * hy_dx
        q3 = K[EDY] * PSIE[3, p] + K[EGY] * hx_dy
        PSIE[0, p], PSIE[1, p], PSIE[2, p], PSIE[3, p] = q0, q1, q2, q3
        ce = CE[p]
        ex = ex + ce * (hz_dy + q0 - hy_dz)
        ey = ey + ce * (hx_dz - hz_dx - q1)
        ez = ez + ce * (hy_dx + q2 - hx_dy - q3)
        F[0, p], F[1, p], F[2, p] = ex, ey, ez
        PSIH[0, p], PSIH[1, p], PSIH[2, p], PSIH[3, p] = p0, p1, p2, p3
        return (ex, ey, ez), (hx, hy, hz)

    routes = [
        (dn_x, up_x, sxd, rxd, (row - 1, col)),
        (up_x, dn_x, sxu, rxu, (row + 1, col)),
        (dn_y, up_y, syd, ryd, (row, col - 1)),
        (up_y, dn_y, syu, ryu, (row, col + 1)),
        (ca_out, ca_in, sca, rca, (row + 1, col - 1)),
        (ca_in, ca_out, scb, rcb, (row - 1, col + 1)),
    ]

    def message(i, n, c):
        _, _, src, dst, device = routes[i]
        return pltpu.make_async_remote_copy(
            src_ref=src.at[n, c], dst_ref=dst.at[n, c],
            send_sem=hs_sem.at[i], recv_sem=hr_sem.at[lax.rem(n, 2), c, i],
            device_id=device, device_id_type=MESH,
        )

    def arrived(n, c):
        for i in range(6):
            pl.when(routes[i][1])(lambda: message(i, n, c).wait_recv())
        before = lax.max(c - 1, 0)
        yu = ryu[n, c] - K[CXU] * wide(rcb[n, c])
        cas = wide(rca[n, before]), wide(rca[n, c])
        return (ryd[n, before], ryd[n, c]), yu, cas

    def send(n, c, pd, pu, pb):
        syd[n, c], syu[n, c], sca[n, c], scb[n, c] = pd, pu, pd[7:8, :], pb[0:1, :]
        for i in (4, 5, 0, 1, 2, 3):
            pl.when(routes[i][0])(lambda: message(i, n, c).start())

    def bytes_of(ref, sem):
        pltpu.make_async_copy(ref, ref, sem).wait()

    def all_left():
        for i in range(6):
            pl.when(routes[i][0])(lambda: bytes_of(routes[i][2], hs_sem.at[i]))

    def mode_copy(j, first, count):
        dest = lax.rem(row + j, n_row)
        return pltpu.make_async_remote_copy(
            src_ref=M.at[dest, pl.ds(first, count)],
            dst_ref=W.at[pl.ds(row * modes_here + first, count)],
            send_sem=bs_sem.at[0], recv_sem=br_sem.at[0],
            device_id=(dest, col), device_id_type=MESH,
        )

    def mode_piece(k):
        half = modes_here // 2
        mode_copy(1 + 2 * lax.div(k, 2), lax.rem(k, 2) * half, half).start()

    for copy in loads:
        copy.wait()
    pl.semaphore_wait(barrier, greeted)
    none = (zero, zero, zero)

    def opening(c, carry):
        E, H = carry
        pd = pu = pb = zero
        for i in range(deep):
            z = c * deep + i
            p = z + pad
            ahead = F[0, p], F[1, p], F[2, p]
            pd = pack_e(0, c, i, ahead, pd)
            pu, pb = finish_h(0, c, i, z - 1, E, H, False, ahead[0], ahead[1], pu, pb)
            E, H = ahead, (F[3, p], F[4, p], F[5, p])
        send(0, c, pd, pu, pb)
        return E, H

    lax.fori_loop(0, chunks, opening, (none, none))
    for k in range(3):
        CAR[k] = zero
    bytes_of(M, own_sem.at[0])
    for j in range(2, n_row, 2):
        mode_copy(j, 0, modes_here).start()
    mode_piece(n_row - 1)

    @pl.loop(0, STEPS - 1)
    def _(n):
        @pl.when(n < n_row - 1)
        def _():
            mode_piece(n)

        @pl.loop(0, chunks)
        def _(c):
            yds, yu, cas = arrived(n, c)
            pd = pu = pb = zero
            below = c * deep - (n + 2) + pad
            E = F[0, below], F[1, below], F[2, below]
            H = CAR[0], CAR[1], CAR[2]
            for i in range(deep):
                z = c * deep - (n + 1) + i
                E2, H2 = electric(n, c, i, z, yds, yu, cas, H[0], H[1])
                pd = pack_e(n + 1, c, i, E2, pd)
                pu, pb = finish_h(n + 1, c, i, z - 1, E, H, True, E2[0], E2[1], pu, pb)
                E, H = E2, H2
            for k, value in enumerate(H):
                CAR[k] = value
            send(n + 1, c, pd, pu, pb)

    def closing(c, carry):
        n = STEPS - 1
        yds, yu, cas = arrived(n, c)
        for i in range(deep):
            z = c * deep - (n + 1) + i
            _, H = electric(n, c, i, z, yds, yu, cas, carry[0], carry[1])
            F[3, z + pad], F[4, z + pad], F[5, z + pad] = H
            carry = H[0], H[1]
        return carry

    lax.fori_loop(0, chunks, closing, (zero, zero))

    count = snap.shape[0]
    rank = modes_here * n_row

    @pl.loop(0, count // 8)
    def _(g):
        for k in range(8):
            plane = snap[g * 8 + k]
            W[rank + g * 8 + k] = F[lax.div(plane, nz), pad + lax.rem(plane, nz)]

    W[pl.ds(row * modes_here, modes_here)] = M[row]

    elsewhere = W.at[0:rank - modes_here]
    bytes_of(elsewhere, br_sem.at[0])

    both = jnp.zeros((count, rank + count), f32)
    for x in range(8):
        both = both + lax.dot_general(
            W[rank:rank + count, x, :], W[:, x, :], (((1,), (1,)), ((), ())),
            precision=lax.Precision.HIGHEST, preferred_element_type=f32,
        )
    R[0:8] = both[:, :rank].reshape(8, 8, 128)
    gram = both[:, rank:] * (1.0 / (full_x * full_y))
    gram = jnp.concatenate([gram, jnp.zeros((count, 128 - count), f32)], axis=1)
    R[8:16] = gram.reshape(8, 8, 128)

    piece = 16 // n_a
    RA[a_me] = R[pl.ds(a_me * piece, piece)]

    def scatter(j):
        m = lax.rem(a_me + j, n_a)
        return pltpu.make_async_remote_copy(
            src_ref=R.at[pl.ds(m * piece, piece)], dst_ref=RA.at[a_me],
            send_sem=as_sem.at[0], recv_sem=ar_sem.at[0],
            device_id=a_device(m), device_id_type=MESH,
        )

    def exchange(j):
        m = lax.rem(b_me + j, n_b)
        return pltpu.make_async_remote_copy(
            src_ref=PB.at[b_me], dst_ref=PB.at[b_me],
            send_sem=ps_sem.at[0], recv_sem=pr_sem.at[0],
            device_id=b_device(m), device_id_type=MESH,
        )

    def gather(j):
        m = lax.rem(a_me + j, n_a)
        return pltpu.make_async_remote_copy(
            src_ref=G.at[a_me], dst_ref=G.at[a_me],
            send_sem=gs_sem.at[0], recv_sem=gr_sem.at[0],
            device_id=a_device(m), device_id_type=MESH,
        )

    def run(make, n, land, sem, meanwhile=None):
        @pl.loop(1, n)
        def _(j):
            make(j).start()

        if meanwhile is not None:
            meanwhile()
        bytes_of(land.at[0:n - 1], sem.at[0])

    def total(ref, n):
        out = ref[0]
        for m in range(1, n):
            out = out + ref[m]
        return out

    run(scatter, n_a, RA, ar_sem, all_left)
    PB[b_me] = total(RA, n_a)
    run(exchange, n_b, PB, pr_sem)
    G[a_me] = total(PB, n_b)
    run(gather, n_a, G, gr_sem)
    whole = G[...].reshape(16, 8, 128)
    coef_out[...] = whole[0:8].reshape(64, 128)
    gram_out[...] = whole[8:16].reshape(64, 128)[:, :64]


    bytes_of(elsewhere, bs_sem.at[0])
    bytes_of(RA.at[0:n_a - 1], as_sem.at[0])
    bytes_of(PB.at[0:n_b - 1], ps_sem.at[0])
    bytes_of(G.at[0:n_a - 1], gs_sem.at[0])


def solution(mesh):
    n_row, n_col = mesh.shape["row"], mesh.shape["col"]
    n_a, n_b = n_row * 2, n_col // 2
    piece = 16 // n_a

    def shards(e_field, h_field, e_coef, basis, pml_width, snap_index):
        nz = e_coef.shape[0]
        rank = basis.shape[0] * n_row
        count = snap_index.shape[0]
        dma = pltpu.SemaphoreType.DMA
        hbm = pl.BlockSpec(memory_space=pl.ANY)
        smem = pl.BlockSpec(memory_space=pltpu.SMEM)
        vmem = pl.BlockSpec(memory_space=pltpu.VMEM)
        chunks = 6 if nz == 64 else 2
        deep = -(-(nz + STEPS) // chunks)
        tall = deep * chunks + STEPS
        rows = pltpu.VMEM((STEPS, chunks, -(-deep // 4) * 8, 128), f32)
        tiles = pltpu.VMEM((STEPS, chunks, 8, 128), f32)
        lines = pltpu.VMEM((STEPS, chunks, 1, 128), f32)
        fields, coefficients, gram = pl.pallas_call(
            functools.partial(kernel, n_row, n_col, nz, chunks),
            out_shape=(
                pltpu.VMEM((6, tall, 8, 128), f32),
                pltpu.VMEM((count, rank), f32),
                pltpu.VMEM((count, count), f32),
            ),
            in_specs=[hbm, hbm, hbm, hbm, smem, smem],
            out_specs=(vmem, vmem, vmem),
            scratch_shapes=[
                pltpu.VMEM((tall, 8, 128), f32),
                pltpu.VMEM((3, tall, 8, 128), f32),
                pltpu.VMEM((4, tall, 8, 128), f32),
                pltpu.VMEM((4, tall, 8, 128), f32),
                pltpu.VMEM((14, 8, 128), f32),
                pltpu.VMEM((3, 8, 128), f32),
                rows, rows, tiles, tiles, lines, lines,
                rows, rows, tiles, tiles, lines, lines,
                pltpu.VMEM((rank + count, 8, 128), f32),
                pltpu.VMEM((n_row, basis.shape[0], 8, 128), f32),
                pltpu.VMEM((16, 8, 128), f32),
                pltpu.VMEM((n_a, piece, 8, 128), f32),
                pltpu.VMEM((n_b, piece, 8, 128), f32),
                pltpu.VMEM((n_a, piece, 8, 128), f32),
                dma((3,)), dma((6,)), dma((2, chunks, 6)),
                dma((1,)), dma((1,)), dma((1,)),
                dma((1,)), dma((1,)), dma((1,)), dma((1,)), dma((1,)), dma((1,)),
            ],
            compiler_params=pltpu.CompilerParams(collective_id=0, has_side_effects=True),
            name="yee",
        )(e_field, h_field, e_coef, basis, pml_width, snap_index)

        def write(F, coef, gram, e_out, h_out, coef_out, gram_out, sem):
            inner = slice(STEPS, STEPS + nz)
            copies = [
                pltpu.make_async_copy(F.at[0:3, inner], e_out, sem.at[0]),
                pltpu.make_async_copy(F.at[3:6, inner], h_out, sem.at[1]),
                pltpu.make_async_copy(coef, coef_out, sem.at[2]),
                pltpu.make_async_copy(gram, gram_out, sem.at[3]),
            ]
            for copy in copies:
                copy.start()
            for copy in copies:
                copy.wait()

        return pl.pallas_call(
            write,
            out_shape=(
                jax.ShapeDtypeStruct(e_field.shape, f32),
                jax.ShapeDtypeStruct(h_field.shape, f32),
                jax.ShapeDtypeStruct((count, rank), f32),
                jax.ShapeDtypeStruct((count, count), f32),
            ),
            in_specs=[vmem, vmem, vmem],
            out_specs=(hbm, hbm, hbm, hbm),
            scratch_shapes=[dma((4,))],
            name="write",
        )(*[pltpu.with_memory_space_constraint(v, pltpu.VMEM) for v in (fields, coefficients, gram)])

    return jax.shard_map(
        shards,
        mesh=mesh,
        in_specs=(
            P(None, None, "row", "col"),
            P(None, None, "row", "col"),
            P(None, "row", "col"),
            P("row", None, "col"),
            P(),
            P(),
        ),
        out_specs=(P(None, None, "row", "col"), P(None, None, "row", "col"), P(), P()),
        check_vma=False,
    )
```

```python
import functools

import jax
import jax.numpy as jnp
from jax import lax
from jax.experimental import pallas as pl
from jax.experimental.pallas import tpu as pltpu
from jax.sharding import PartitionSpec as P

STEPS = 8
time_step = 0.5
sigma_top = 4.0
alpha_shift = 0.05
MESH = pl.DeviceIdType.MESH
TILE = (8, 128)
f32 = jnp.float32


def absorber(positions, total, low, high):
    depth = jnp.maximum(
        jnp.maximum((low - positions) / low, (positions - (total - 1.0 - high)) / high), 0.0
    )
    sigma = sigma_top * (depth * depth * depth)
    damp = jnp.exp(-(sigma + alpha_shift) * time_step)
    gain = sigma / (sigma + alpha_shift) * (damp - 1.0)
    return damp, gain


def kernel(
    n_row, n_col, nz, chunks,
    e_in, h_in, c_in, basis, pml, snap,
    F, coef_out, gram_out,
    CE, HP, PSIH, PSIE, K, CAR,
    sxd, sxu, syd, syu, sca, scb,
    rxd, rxu, ryd, ryu, rca, rcb,
    W, M, R, RA, PB, G,
    in_sem, hs_sem, hr_sem, bs_sem, br_sem, own_sem,
    as_sem, ar_sem, ps_sem, pr_sem, gs_sem, gr_sem,
):
    pad = STEPS
    deep = -(-(nz + pad) // chunks)
    tall = F.shape[1]
    row = lax.axis_index("row")
    col = lax.axis_index("col")
    n_a, n_b = n_row * 2, n_col // 2
    y_lo = lax.rem(lax.div(col, 2), 2)
    a_me = row * 2 + y_lo
    b_me = lax.div(col, 4) * 2 + lax.rem(col, 2)

    def a_device(m):
        return (lax.div(m, 2), lax.div(col, 4) * 4 + lax.rem(m, 2) * 2 + lax.rem(col, 2))

    def b_device(m):
        return (row, lax.div(m, 2) * 4 + y_lo * 2 + lax.rem(m, 2))

    loads = [
        pltpu.make_async_copy(e_in, F.at[0:3, pad:pad + nz], in_sem.at[0]),
        pltpu.make_async_copy(h_in, F.at[3:6, pad:pad + nz], in_sem.at[1]),
        pltpu.make_async_copy(c_in, CE.at[pad:pad + nz], in_sem.at[2]),
    ]
    for copy in loads:
        copy.start()
    modes_here = basis.shape[0]

    def modes_for(dest):
        return pltpu.make_async_copy(basis.at[:, 8 * dest:8 * dest + 8, :], M.at[dest], own_sem.at[0])

    for dest in range(n_row):
        modes_for(dest).start()

    barrier = pltpu.get_barrier_semaphore()

    def greet(device):
        pl.semaphore_signal(barrier, inc=1, device_id=device, device_id_type=MESH)

    @pl.loop(1, n_a)
    def _(j):
        greet(a_device(lax.rem(a_me + j, n_a)))

    @pl.loop(1, n_b)
    def _(j):
        greet(b_device(lax.rem(b_me + j, n_b)))

    up_x, dn_x = row < n_row - 1, row > 0
    up_y, dn_y = col < n_col - 1, col > 0
    ca_out, ca_in = up_x & dn_y, dn_x & up_y

    @pl.when(up_y)
    def _():
        greet((row, col + 1))

    @pl.when(dn_y)
    def _():
        greet((row, col - 1))

    @pl.when(ca_out)
    def _():
        greet((row + 1, col - 1))

    @pl.when(ca_in)
    def _():
        greet((row - 1, col + 1))

    greeted = n_a - 1 + n_b - 1
    for flag in (up_y, dn_y, ca_out, ca_in):
        greeted = greeted + flag.astype(jnp.int32)

    sub = lax.broadcasted_iota(jnp.int32, TILE, 0)
    lane = lax.broadcasted_iota(jnp.int32, TILE, 1)
    w = [jnp.full(TILE, pml[i], jnp.int32).astype(f32) for i in range(4)]
    x_pos = (row * 8 + sub).astype(f32)
    y_pos = (col * 128 + lane).astype(f32)
    full_x, full_y = float(n_row * 8), float(n_col * 128)
    hdx, hgx = absorber(x_pos + 0.5, full_x, w[0], w[1])
    hdy, hgy = absorber(y_pos + 0.5, full_y, w[2], w[3])
    edx, egx = absorber(x_pos, full_x, w[0], w[1])
    edy, egy = absorber(y_pos, full_y, w[2], w[3])
    _, gxm = absorber((row * 8 - 1 + 0 * sub).astype(f32) + 0.5, full_x, w[0], w[1])
    _, gym = absorber((col * 128 - 1 + 0 * lane).astype(f32) + 0.5, full_y, w[2], w[3])
    s7, s0, l127, l0 = sub == 7, sub == 0, lane == 127, lane == 0
    zero = jnp.zeros(TILE, f32)
    coeffs = [
        hdx, hgx, hdy, hgy, edx, egx, edy, egy,
        jnp.where(s7, 0.5 * (1.0 + hgx), zero), jnp.where(s7, hgx, zero),
        jnp.where(l127, 0.5 * (1.0 + hgy), zero), jnp.where(l127, hgy, zero),
        0.5 * (1.0 + gxm) * dn_x.astype(f32), 0.5 * (1.0 + gym) * dn_y.astype(f32),
    ]
    for i, value in enumerate(coeffs):
        K[i] = value
    HDX, HGX, HDY, HGY, EDX, EGX, EDY, EGY, CXU, PXU, CYU, PYU, CXD, CYD = range(14)

    @pl.loop(0, tall)
    def _(z):
        for i in range(4):
            PSIE[i, z] = zero
            PSIH[i, z] = zero

    for beyond in (*range(pad), *range(pad + nz, tall)):
        CE[beyond] = zero
        for i in range(6):
            F[i, beyond] = zero

    def clear(ref, wanted):
        @pl.when(wanted)
        def _():
            @pl.loop(0, STEPS)
            def _(n):
                ref[n] = jnp.zeros(ref.shape[1:], f32)

    clear(rxd, ~up_x)
    clear(rxu, ~dn_x)
    clear(ryd, ~up_y)
    clear(ryu, ~dn_y)
    clear(rca, ~ca_in)
    clear(rcb, ~ca_out)

    def wide(v):
        return jnp.broadcast_to(v, TILE)

    def roll_l(v, by):
        by = by % 128
        return pltpu.roll(v, by, 1) if by else v

    def roll_s(v, by):
        return pltpu.roll(v, by, 0)

    def partial_h(E, H, psi, ex_next, ey_next):
        ex, ey, ez = E
        hx, hy, hz = H
        ez_dy = jnp.where(l127, 0.0, roll_l(ez, 127)) - ez
        ex_dy = jnp.where(l127, 0.0, roll_l(ex, 127)) - ex
        ez_dx = jnp.where(s7, 0.0, roll_s(ez, 7)) - ez
        ey_dx = jnp.where(s7, 0.0, roll_s(ey, 7)) - ey
        ey_dz = ey_next - ey
        ex_dz = ex_next - ex
        p0, p1, p2, p3 = K[HGY] * ez_dy, K[HGX] * ez_dx, K[HGX] * ey_dx, K[HGY] * ex_dy
        if psi is not None:
            p0, p1 = K[HDY] * psi[0] + p0, K[HDX] * psi[1] + p1
            p2, p3 = K[HDX] * psi[2] + p2, K[HDY] * psi[3] + p3
        hx = hx - time_step * (ez_dy + p0 - ey_dz)
        hy = hy - time_step * (ex_dz - ez_dx - p1)
        hz = hz - time_step * (ey_dx + p2 - ex_dy - p3)
        return (hx, hy, hz), (p0, p1, p2, p3)

    def put(packed, i, low, high):
        if low is not None:
            packed = jnp.where(lane == i, low, packed)
        return jnp.where(lane == 64 + i, high, packed)

    def pack_e(n, c, i, E, pd):
        ex, ey, ez = E
        sxd[n, c, 2 * i:2 * i + 1, :] = ey[0:1, :]
        sxd[n, c, 2 * i + 1:2 * i + 2, :] = ez[0:1, :]
        return put(pd, i, roll_l(ex, i), roll_l(ez, 64 + i))

    def finish_h(n, c, i, z, E, H, later, ex_next, ey_next, pu, pb):
        psi = tuple(PSIH[k, z + pad] for k in range(4)) if later else None
        H, psi = partial_h(E, H, psi, ex_next, ey_next)
        for k in range(3):
            HP[k, z + pad] = H[k]
        for k in range(4):
            PSIH[k, z + pad] = psi[k]
        sxu[n, c, 2 * i:2 * i + 1, :] = H[1][7:8, :]
        sxu[n, c, 2 * i + 1:2 * i + 2, :] = H[2][7:8, :]
        pu = put(pu, i, roll_l(H[0], i - 127), roll_l(H[2], 64 + i - 127))
        pb = put(pb, i, None, roll_l(E[1], 64 + i - 127))
        return pu, pb

    def electric(n, c, i, z, yds, yu, cas, hx_prev, hy_prev):
        p = z + pad
        ex, ey, ez = F[0, p], F[1, p], F[2, p]
        hx, hy, hz = HP[0, p], HP[1, p], HP[2, p]
        p0, p1, p2, p3 = PSIH[0, p], PSIH[1, p], PSIH[2, p], PSIH[3, p]
        if i == 0:
            k, j = lax.max(c - 1, 0), deep - 1
        else:
            k, j = c, i - 1
        yd, ca = yds[i > 0], cas[i > 0]
        ey8 = wide(rxd[n, k, 2 * j:2 * j + 1, :])
        ez8 = wide(rxd[n, k, 2 * j + 1:2 * j + 2, :])
        ex128, ez128 = roll_l(yd, 127 - j), roll_l(yd, 63 - j)
        if i <= pad:
            hx_prev = jnp.where(z == 0, zero, hx_prev)
            hy_prev = jnp.where(z == 0, zero, hy_prev)
        hy = hy + K[CXU] * ez8
        p1 = p1 + K[PXU] * ez8
        hx = hx - K[CYU] * ez128
        p0 = p0 + K[PYU] * ez128
        hz = hz - K[CXU] * ey8 + K[CYU] * ex128
        p2 = p2 + K[PXU] * ey8
        p3 = p3 + K[PYU] * ex128
        hy_m = wide(rxu[n, c, 2 * i:2 * i + 1, :]) + K[CXD] * ez
        hz_m = wide(rxu[n, c, 2 * i + 1:2 * i + 2, :]) - K[CXD] * ey
        hz_m = hz_m + K[CYU] * roll_l(ca, 127 - j)
        hx_w = roll_l(yu, -i) - K[CYD] * ez
        hz_w = roll_l(yu, 64 - i) + K[CYD] * ex
        hz_dy = hz - jnp.where(l0, hz_w, roll_l(hz, 1))
        hx_dy = hx - jnp.where(l0, hx_w, roll_l(hx, 1))
        hz_dx = hz - jnp.where(s0, hz_m, roll_s(hz, 1))
        hy_dx = hy - jnp.where(s0, hy_m, roll_s(hy, 1))
        hy_dz = hy - hy_prev
        hx_dz = hx - hx_prev
        q0 = K[EDY] * PSIE[0, p] + K[EGY] * hz_dy
        q1 = K[EDX] * PSIE[1, p] + K[EGX] * hz_dx
        q2 = K[EDX] * PSIE[2, p] + K[EGX] * hy_dx
        q3 = K[EDY] * PSIE[3, p] + K[EGY] * hx_dy
        PSIE[0, p], PSIE[1, p], PSIE[2, p], PSIE[3, p] = q0, q1, q2, q3
        ce = CE[p]
        ex = ex + ce * (hz_dy + q0 - hy_dz)
        ey = ey + ce * (hx_dz - hz_dx - q1)
        ez = ez + ce * (hy_dx + q2 - hx_dy - q3)
        F[0, p], F[1, p], F[2, p] = ex, ey, ez
        PSIH[0, p], PSIH[1, p], PSIH[2, p], PSIH[3, p] = p0, p1, p2, p3
        return (ex, ey, ez), (hx, hy, hz)

    routes = [
        (dn_x, up_x, sxd, rxd, (row - 1, col)),
        (up_x, dn_x, sxu, rxu, (row + 1, col)),
        (dn_y, up_y, syd, ryd, (row, col - 1)),
        (up_y, dn_y, syu, ryu, (row, col + 1)),
        (ca_out, ca_in, sca, rca, (row + 1, col - 1)),
        (ca_in, ca_out, scb, rcb, (row - 1, col + 1)),
    ]

    def message(i, n, c):
        _, _, src, dst, device = routes[i]
        return pltpu.make_async_remote_copy(
            src_ref=src.at[n, c], dst_ref=dst.at[n, c],
            send_sem=hs_sem.at[i], recv_sem=hr_sem.at[lax.rem(n, 2), c, i],
            device_id=device, device_id_type=MESH,
        )

    def arrived(n, c):
        for i in range(6):
            pl.when(routes[i][1])(lambda: message(i, n, c).wait_recv())
        before = lax.max(c - 1, 0)
        yu = ryu[n, c] - K[CXU] * wide(rcb[n, c])
        cas = wide(rca[n, before]), wide(rca[n, c])
        return (ryd[n, before], ryd[n, c]), yu, cas

    def send(n, c, pd, pu, pb):
        syd[n, c], syu[n, c], sca[n, c], scb[n, c] = pd, pu, pd[7:8, :], pb[0:1, :]
        for i in (4, 5, 0, 1, 2, 3):
            pl.when(routes[i][0])(lambda: message(i, n, c).start())

    def bytes_of(ref, sem):
        pltpu.make_async_copy(ref, ref, sem).wait()

    def all_left():
        for i in range(6):
            pl.when(routes[i][0])(lambda: bytes_of(routes[i][2], hs_sem.at[i]))

    def mode_copy(j, first, count):
        dest = lax.rem(row + j, n_row)
        return pltpu.make_async_remote_copy(
            src_ref=M.at[dest, pl.ds(first, count)],
            dst_ref=W.at[pl.ds(row * modes_here + first, count)],
            send_sem=bs_sem.at[0], recv_sem=br_sem.at[0],
            device_id=(dest, col), device_id_type=MESH,
        )

    def mode_piece(k):
        part = modes_here // 4
        mode_copy(1 + 2 * lax.div(k, 4), lax.rem(k, 4) * part, part).start()

    for copy in loads:
        copy.wait()
    pl.semaphore_wait(barrier, greeted)
    none = (zero, zero, zero)

    def opening(c, carry):
        E, H = carry
        pd = pu = pb = zero
        for i in range(deep):
            z = c * deep + i
            p = z + pad
            ahead = F[0, p], F[1, p], F[2, p]
            pd = pack_e(0, c, i, ahead, pd)
            pu, pb = finish_h(0, c, i, z - 1, E, H, False, ahead[0], ahead[1], pu, pb)
            E, H = ahead, (F[3, p], F[4, p], F[5, p])
        send(0, c, pd, pu, pb)
        return E, H

    lax.fori_loop(0, chunks, opening, (none, none))
    for k in range(3):
        CAR[k] = zero
    bytes_of(M, own_sem.at[0])
    for j in range(2, n_row, 2):
        mode_copy(j, 0, modes_here).start()
    mode_piece(2 * n_row - 2)
    mode_piece(2 * n_row - 1)

    @pl.loop(0, STEPS - 1)
    def _(n):

        @pl.loop(0, chunks)
        def _(c):
            yds, yu, cas = arrived(n, c)
            pd = pu = pb = zero
            below = c * deep - (n + 2) + pad
            E = F[0, below], F[1, below], F[2, below]
            H = CAR[0], CAR[1], CAR[2]
            for i in range(deep):
                z = c * deep - (n + 1) + i
                E2, H2 = electric(n, c, i, z, yds, yu, cas, H[0], H[1])
                pd = pack_e(n + 1, c, i, E2, pd)
                pu, pb = finish_h(n + 1, c, i, z - 1, E, H, True, E2[0], E2[1], pu, pb)
                E, H = E2, H2
            for k, value in enumerate(H):
                CAR[k] = value
            send(n + 1, c, pd, pu, pb)

            @pl.when(lax.rem(c, 3) == 2)
            def _():
                mode_piece(2 * n + lax.div(c, 3))

    def closing(c, carry):
        n = STEPS - 1
        yds, yu, cas = arrived(n, c)
        for i in range(deep):
            z = c * deep - (n + 1) + i
            _, H = electric(n, c, i, z, yds, yu, cas, carry[0], carry[1])
            F[3, z + pad], F[4, z + pad], F[5, z + pad] = H
            carry = H[0], H[1]
        return carry

    lax.fori_loop(0, chunks, closing, (zero, zero))

    count = snap.shape[0]
    rank = modes_here * n_row

    @pl.loop(0, count // 8)
    def _(g):
        for k in range(8):
            plane = snap[g * 8 + k]
            W[rank + g * 8 + k] = F[lax.div(plane, nz), pad + lax.rem(plane, nz)]

    W[pl.ds(row * modes_here, modes_here)] = M[row]

    elsewhere = W.at[0:rank - modes_here]
    bytes_of(elsewhere, br_sem.at[0])

    both = jnp.zeros((count, rank + count), f32)
    for x in range(8):
        both = both + lax.dot_general(
            W[rank:rank + count, x, :], W[:, x, :], (((1,), (1,)), ((), ())),
            precision=lax.Precision.HIGHEST, preferred_element_type=f32,
        )
    R[0:8] = both[:, :rank].reshape(8, 8, 128)
    gram = both[:, rank:] * (1.0 / (full_x * full_y))
    gram = jnp.concatenate([gram, jnp.zeros((count, 128 - count), f32)], axis=1)
    R[8:16] = gram.reshape(8, 8, 128)

    piece = 16 // n_a
    RA[a_me] = R[pl.ds(a_me * piece, piece)]

    def scatter(j):
        m = lax.rem(a_me + j, n_a)
        return pltpu.make_async_remote_copy(
            src_ref=R.at[pl.ds(m * piece, piece)], dst_ref=RA.at[a_me],
            send_sem=as_sem.at[0], recv_sem=ar_sem.at[0],
            device_id=a_device(m), device_id_type=MESH,
        )

    def exchange(j):
        m = lax.rem(b_me + j, n_b)
        return pltpu.make_async_remote_copy(
            src_ref=PB.at[b_me], dst_ref=PB.at[b_me],
            send_sem=ps_sem.at[0], recv_sem=pr_sem.at[0],
            device_id=b_device(m), device_id_type=MESH,
        )

    def gather(j):
        m = lax.rem(a_me + j, n_a)
        return pltpu.make_async_remote_copy(
            src_ref=G.at[a_me], dst_ref=G.at[a_me],
            send_sem=gs_sem.at[0], recv_sem=gr_sem.at[0],
            device_id=a_device(m), device_id_type=MESH,
        )

    def run(make, n, land, sem, meanwhile=None):
        @pl.loop(1, n)
        def _(j):
            make(j).start()

        if meanwhile is not None:
            meanwhile()
        bytes_of(land.at[0:n - 1], sem.at[0])

    def total(ref, n):
        out = ref[0]
        for m in range(1, n):
            out = out + ref[m]
        return out

    run(scatter, n_a, RA, ar_sem, all_left)
    PB[b_me] = total(RA, n_a)
    run(exchange, n_b, PB, pr_sem)
    G[a_me] = total(PB, n_b)
    run(gather, n_a, G, gr_sem)
    whole = G[...].reshape(16, 8, 128)
    coef_out[...] = whole[0:8].reshape(64, 128)
    gram_out[...] = whole[8:16].reshape(64, 128)[:, :64]


    bytes_of(elsewhere, bs_sem.at[0])
    bytes_of(RA.at[0:n_a - 1], as_sem.at[0])
    bytes_of(PB.at[0:n_b - 1], ps_sem.at[0])
    bytes_of(G.at[0:n_a - 1], gs_sem.at[0])


def solution(mesh):
    n_row, n_col = mesh.shape["row"], mesh.shape["col"]
    n_a, n_b = n_row * 2, n_col // 2
    piece = 16 // n_a

    def shards(e_field, h_field, e_coef, basis, pml_width, snap_index):
        nz = e_coef.shape[0]
        rank = basis.shape[0] * n_row
        count = snap_index.shape[0]
        dma = pltpu.SemaphoreType.DMA
        hbm = pl.BlockSpec(memory_space=pl.ANY)
        smem = pl.BlockSpec(memory_space=pltpu.SMEM)
        vmem = pl.BlockSpec(memory_space=pltpu.VMEM)
        chunks = 6 if nz == 64 else 2
        deep = -(-(nz + STEPS) // chunks)
        tall = deep * chunks + STEPS
        rows = pltpu.VMEM((STEPS, chunks, -(-deep // 4) * 8, 128), f32)
        tiles = pltpu.VMEM((STEPS, chunks, 8, 128), f32)
        lines = pltpu.VMEM((STEPS, chunks, 1, 128), f32)
        fields, coefficients, gram = pl.pallas_call(
            functools.partial(kernel, n_row, n_col, nz, chunks),
            out_shape=(
                pltpu.VMEM((6, tall, 8, 128), f32),
                pltpu.VMEM((count, rank), f32),
                pltpu.VMEM((count, count), f32),
            ),
            in_specs=[hbm, hbm, hbm, hbm, smem, smem],
            out_specs=(vmem, vmem, vmem),
            scratch_shapes=[
                pltpu.VMEM((tall, 8, 128), f32),
                pltpu.VMEM((3, tall, 8, 128), f32),
                pltpu.VMEM((4, tall, 8, 128), f32),
                pltpu.VMEM((4, tall, 8, 128), f32),
                pltpu.VMEM((14, 8, 128), f32),
                pltpu.VMEM((3, 8, 128), f32),
                rows, rows, tiles, tiles, lines, lines,
                rows, rows, tiles, tiles, lines, lines,
                pltpu.VMEM((rank + count, 8, 128), f32),
                pltpu.VMEM((n_row, basis.shape[0], 8, 128), f32),
                pltpu.VMEM((16, 8, 128), f32),
                pltpu.VMEM((n_a, piece, 8, 128), f32),
                pltpu.VMEM((n_b, piece, 8, 128), f32),
                pltpu.VMEM((n_a, piece, 8, 128), f32),
                dma((3,)), dma((6,)), dma((2, chunks, 6)),
                dma((1,)), dma((1,)), dma((1,)),
                dma((1,)), dma((1,)), dma((1,)), dma((1,)), dma((1,)), dma((1,)),
            ],
            compiler_params=pltpu.CompilerParams(collective_id=0, has_side_effects=True),
            name="yee",
        )(e_field, h_field, e_coef, basis, pml_width, snap_index)

        def write(F, coef, gram, e_out, h_out, coef_out, gram_out, sem):
            inner = slice(STEPS, STEPS + nz)
            copies = [
                pltpu.make_async_copy(F.at[0:3, inner], e_out, sem.at[0]),
                pltpu.make_async_copy(F.at[3:6, inner], h_out, sem.at[1]),
                pltpu.make_async_copy(coef, coef_out, sem.at[2]),
                pltpu.make_async_copy(gram, gram_out, sem.at[3]),
            ]
            for copy in copies:
                copy.start()
            for copy in copies:
                copy.wait()

        return pl.pallas_call(
            write,
            out_shape=(
                jax.ShapeDtypeStruct(e_field.shape, f32),
                jax.ShapeDtypeStruct(h_field.shape, f32),
                jax.ShapeDtypeStruct((count, rank), f32),
                jax.ShapeDtypeStruct((count, count), f32),
            ),
            in_specs=[vmem, vmem, vmem],
            out_specs=(hbm, hbm, hbm, hbm),
            scratch_shapes=[dma((4,))],
            name="write",
        )(*[pltpu.with_memory_space_constraint(v, pltpu.VMEM) for v in (fields, coefficients, gram)])

    return jax.shard_map(
        shards,
        mesh=mesh,
        in_specs=(
            P(None, None, "row", "col"),
            P(None, None, "row", "col"),
            P(None, "row", "col"),
            P("row", None, "col"),
            P(),
            P(),
        ),
        out_specs=(P(None, None, "row", "col"), P(None, None, "row", "col"), P(), P()),
        check_vma=False,
    )
```
